512 devices in a mesh: row: 16 (over z), col: 32 (over x, y, core).
Axes of the slice: x: 4, y: 4, z: 16, core: 2. Of those that a mesh axis runs over, the one named last changes fastest.
Arguments:
- points: float32 [8, 32768], P(None, ('row', 'col')), may hold values from -15 to 15
- noise_level: float32 [32768], P('row'), may hold values from 0.5 to 2
- right_sides: float32 [64, 32768], P(None, 'row'), may hold values from -6 to 6
Outputs:
- solution: float32 [64, 32768], P(None, 'row')
- residual: float32 [64, 32768], P(None, 'row')
- rel_norms: float32 [64], replicated
The draws below stay inside these ranges and needn't reach their ends.
All inputs are finite; a program needn't handle non-finite values.
Results may differ from the reference program's by a relative error of at most 0.0008.
Values sent between devices are 32-bit elements; how exact they have to be, the bound alone decides.
No kernel may reach another device: no remote copies, remote signals or barrier semaphores. Data moves between devices by JAX's collectives and lax.ppermute only.
A program may use at most 64 MiB of HBM per device.

```python
import math
import jax
import jax.numpy as jnp
from jax import lax

DIM = 8
RHS = 64
ITERS = 2
NPTS = 32768


def block_levels(key, shape, cuts, least, largest):
    loudness, own = 1.0, jax.random.fold_in(key, 6)
    for position, shards_of in cuts:
        draws = jnp.exp(jax.random.uniform(jax.random.fold_in(own, position), (shards_of,), jnp.float32, least / len(cuts), largest / len(cuts)))
        loudness = loudness * jnp.repeat(draws, shape[position] // shards_of).reshape([-1 if axis == position else 1 for axis in range(len(shape))])
    return loudness


def centred(stream_key, shape, scale, most, pieces=(), kind=jnp.bfloat16):
    drawn = jax.random.normal(stream_key, shape, jnp.float32) * scale
    if len(pieces) > 0:
        drawn = block_levels(stream_key, shape, pieces, -0.22, 0.18) * drawn
    return jnp.clip(drawn, min=-most, max=most).astype(kind)


def setup_inputs(seed: int = 0) -> dict:
    arg_keys = jax.random.split(jax.random.key(seed), 4)
    points = centred(arg_keys[0], (DIM, NPTS), 2.5, 15.0, ((1, 512),), jnp.float32)
    noise_level = jnp.clip(jnp.exp(math.log(2.0) - 1.3862944 * jax.random.uniform(arg_keys[1], (NPTS,), jnp.float32) ** block_levels(arg_keys[1], (NPTS,), ((0, 16),), -0.2, 0.2)), 0.5, 2.0)
    right_sides = centred(arg_keys[2], (RHS, NPTS), 1.0, 6.0, ((1, 16),), jnp.float32)
    return {"points": points, "noise_level": noise_level, "right_sides": right_sides}


HIGH = lax.Precision.HIGHEST

def operate(direction, points, sq_norms, noise_level):
    total = points.shape[1]
    tile_rows = math.gcd(total, 2048)
    count = total // tile_rows

    def one_tile(index, image):
        offset = index * tile_rows
        tile_points = lax.dynamic_slice_in_dim(points, offset, tile_rows, 1)
        tile_sq = lax.dynamic_slice_in_dim(sq_norms, offset, tile_rows, 0)
        sq_dist = tile_sq[:, None] + sq_norms[None, :] - 2.0 * jnp.dot(tile_points.T, points, precision=HIGH)
        kernel = jnp.exp(-0.5 * sq_dist)
        piece = lax.dot_general(direction, kernel, (((1,), (1,)), ((), ())), precision=HIGH)
        return lax.dynamic_update_slice_in_dim(image, piece, offset, 1)
    image = lax.fori_loop(0, count, one_tile, jnp.zeros(direction.shape, jnp.float32))
    return image + noise_level[None, :] * direction

def products(first, second):
    return lax.dot_general(first, second, (((1,), (1,)), ((), ())), precision=HIGH)

def solve_sym(matrix, target):
    lower = jnp.linalg.cholesky(0.5 * (matrix + matrix.T))
    return jax.scipy.linalg.cho_solve((lower, True), target)

def reference(points, noise_level, right_sides):
    sq_norms = lax.optimization_barrier(jnp.sum(points * points, axis=0))
    solution = jnp.zeros_like(right_sides)
    residual = right_sides
    direction = right_sides
    gram = products(residual, residual)
    first = gram
    new_gram = gram
    for iteration in range(ITERS):
        image = operate(direction, points, sq_norms, noise_level)
        curv = products(direction, image)
        step_coef = solve_sym(curv, gram)
        solution = solution + jnp.dot(step_coef.T, direction, precision=HIGH)
        residual = residual - jnp.dot(step_coef.T, image, precision=HIGH)
        new_gram = products(residual, residual)
        if iteration + 1 < ITERS:
            dir_coef = solve_sym(gram, new_gram)
            direction = residual + jnp.dot(dir_coef.T, direction, precision=HIGH)
        gram = new_gram
    rel_norms = jnp.sqrt(jnp.diagonal(new_gram) / jnp.diagonal(first))
    return (solution, residual, rel_norms)
```

```python
import functools

import jax
import jax.numpy as jnp
from jax import lax
from jax.experimental import pallas as pl
from jax.experimental.pallas import tpu as pltpu
from jax.sharding import Mesh
from jax.sharding import PartitionSpec as P

COL = ("col_0", "col_1", "col_2")
ROW_COL = ("row", "col_0", "col_1", "col_2")
HIGH = lax.Precision.HIGHEST
F32 = jnp.float32
BF16 = jnp.bfloat16
THETA = 0.5
LANES = 128
HALF = 64
VMEM = pl.BlockSpec(memory_space=pltpu.VMEM)


def lane_of(shape):
    return lax.broadcasted_iota(jnp.int32, shape, len(shape) - 1)


def packed(turned):
    return jnp.concatenate([turned[:32], turned[32:64]], axis=1)


def own_kernel(col_ref, rhs_ref, pts_ref, row_out, col_out):
    turned = rhs_ref[...].T
    odd = lax.rem(col_ref[0], 2) == 1
    block = packed(jnp.where(odd, turned[HALF:], turned[:HALF]))
    pts = jnp.concatenate([pts_ref[...], pts_ref[...]], axis=1)
    unit = jnp.concatenate([block, pts], axis=0)
    for place in range(row_out.shape[0]):
        row_out[place] = unit
    for place in range(col_out.shape[0]):
        col_out[place] = pts


def own_units(col_index, right_sides, points, rows, cols):
    return pl.pallas_call(
        own_kernel,
        grid_spec=pltpu.PrefetchScalarGridSpec(
            num_scalar_prefetch=1,
            grid=(1,),
            in_specs=[
                pl.BlockSpec((HALF, LANES), lambda i, c: (0, c[0] // 2)),
                pl.BlockSpec((8, HALF), lambda i, c: (0, 0)),
            ],
            out_specs=[
                pl.BlockSpec((rows, 40, LANES), lambda i, c: (0, 0, 0)),
                pl.BlockSpec((cols, 8, LANES), lambda i, c: (0, 0, 0)),
            ],
        ),
        out_shape=[
            jax.ShapeDtypeStruct((rows, 40, LANES), F32),
            jax.ShapeDtypeStruct((cols, 8, LANES), F32),
        ],
        name="own_units",
    )(col_index, right_sides, points)


def block_dot(first, second):
    both = lax.dot_general(
        first, second, (((0,), (0,)), ((), ())), precision=HIGH, preferred_element_type=F32
    )
    return both[:HALF, :HALF] + both[HALF:, HALF:]


def packed_kernel(rhs_ref, noise_ref, packed_out, noise_out):
    low = lane_of((32, LANES)) < HALF
    for tile in range(rhs_ref.shape[1] // LANES):
        turned = rhs_ref[:, tile * LANES : (tile + 1) * LANES].T
        noise = noise_ref[:, tile * LANES : (tile + 1) * LANES]
        noise = jnp.broadcast_to(noise, (LANES, LANES)).T
        for part in range(2):
            rows = slice(tile * 64 + part * 32, tile * 64 + part * 32 + 32)
            packed_out[rows] = packed(turned[part * 64 : part * 64 + 64])
            noise_out[rows] = jnp.where(
                low, noise[part * 64 : part * 64 + 32], noise[part * 64 + 32 : part * 64 + 64]
            )


def packed_rows(right_sides, noise_level):
    rows = right_sides.shape[1] // 2
    return pl.pallas_call(
        packed_kernel,
        in_specs=[VMEM] * 2,
        out_specs=[VMEM] * 2,
        out_shape=[jax.ShapeDtypeStruct((rows, LANES), F32)] * 2,
        cost_estimate=pl.CostEstimate(
            flops=4 * 10**9, bytes_accessed=3 * 4 * rows * LANES, transcendentals=0
        ),
        name="packed_rows",
    )(right_sides, noise_level[None, :])


def ordered(units):
    place = lane_of((8, LANES)) // 32
    pieces = []
    for h in range(2):
        for start in range(0, len(units), 4):
            piece = None
            for q in range(4):
                unit = units[start + q]
                if (q - h) % 2:
                    unit = pltpu.roll(unit, 32, 1)
                piece = unit if piece is None else jnp.where(place == q, unit, piece)
            pieces.append(piece)
    return jnp.concatenate(pieces, axis=1)


def rounded(value):
    return value.astype(BF16).astype(F32)


def three_parts(value):
    first = rounded(value)
    rest = value - first
    second = rounded(rest)
    return first, second, rest - second


def augmented(pts, as_rows):
    x1, x2, x3 = three_parts(pts)
    half_sq = -0.5 * jnp.sum(pts * pts, axis=0, keepdims=True)
    s1, s2, s3 = three_parts(half_sq)
    sub = lax.broadcasted_iota(jnp.int32, pts.shape, 0)
    squares = jnp.where(sub == 0, s1, jnp.where(sub == 1, s2, jnp.where(sub == 2, s3, 0.0)))
    ones = jnp.where(sub < 3, 1.0, 0.0)
    zeros = jnp.zeros_like(pts)
    if as_rows:
        blocks = [x1, x1, x2, x2, x1, x3, x2, x3, squares, ones]
    else:
        blocks = [x1, x2, x1, x2, x3, x1, x3, x2, ones, squares]
    return jnp.concatenate(blocks + [zeros] * 6, axis=0)


def apply_kernel_matrix(out_pts, in_pts, values, result, left, right, stack):
    outs = left.shape[0]
    ins = right.shape[1]
    tile = min(256, outs // 2)
    for start in range(0, outs, LANES):
        piece = augmented(out_pts[:, start : start + LANES], True)
        left[start : start + LANES] = piece.T.astype(BF16)
    for start in range(0, ins, 256):
        right[:, start : start + 256] = augmented(in_pts[:, start : start + 256], False).astype(BF16)
    groups = ins // 256
    low = lane_of((LANES, LANES)) < HALF
    for group in range(groups):
        rows = values[group * LANES : (group + 1) * LANES]
        turned = pltpu.roll(rows, HALF, 1)
        for h in range(2):
            top = jnp.where(low, turned if h else rows, 0.0)
            bottom = jnp.where(low, 0.0, rows if h else turned)
            both = jnp.concatenate([top, bottom], axis=0)
            high = both.astype(BF16)
            rest = (both - high.astype(F32)).astype(BF16)
            stack[h * groups + group, :, :LANES] = high
            stack[h * groups + group, :, LANES:] = rest
    result[...] = jnp.zeros_like(result)
    pairs = ins // 256

    def step(index, carry):
        at = pl.multiple_of(lax.div(index, pairs) * tile, tile)
        pair = lax.rem(index, pairs)
        columns = right[:, pl.ds(pl.multiple_of(pair * 256, 256), 256)]
        highs, lows = [], []
        for h in range(2):
            lines = left[pl.ds(h * (outs // 2) + at, tile)]
            kernel = jnp.exp(jnp.dot(lines, columns, preferred_element_type=F32))
            high = kernel.astype(BF16)
            highs.append(high)
            lows.append((kernel - high.astype(F32)).astype(BF16))
        total = result[pl.ds(at, tile)]
        for a in range(2):
            weights = stack[pair * 2 + a]
            cut = slice(a * LANES, (a + 1) * LANES)
            high = jnp.concatenate([highs[0][:, cut], highs[1][:, cut]], axis=1)
            rest = jnp.concatenate([lows[0][:, cut], lows[1][:, cut]], axis=1)
            both = jnp.dot(high, weights, preferred_element_type=F32)
            total = total + both[:, :LANES] + both[:, LANES:]
            total = total + jnp.dot(rest, weights[:, :LANES], preferred_element_type=F32)
        result[pl.ds(at, tile)] = total
        return carry

    lax.fori_loop(0, (outs // 2 // tile) * pairs, step, 0)


def first_product_kernel(unit_ref, col_ref, out_ref, left, right, stack):
    col_pts = ordered([unit_ref[i, 32:] for i in range(unit_ref.shape[0])])
    row_pts = ordered([col_ref[i] for i in range(col_ref.shape[0])])
    values = jnp.concatenate([unit_ref[i, :32] for i in range(unit_ref.shape[0])], axis=0)
    apply_kernel_matrix(row_pts, col_pts, values, out_ref, left, right, stack)


def second_product_kernel(unit_ref, col_ref, raw_ref, rhs_ref, noise_ref, out_ref, image_ref, left, right, stack):
    col_pts = ordered([unit_ref[i, 32:] for i in range(unit_ref.shape[0])])
    row_pts = ordered([col_ref[i] for i in range(col_ref.shape[0])])
    rhs = rhs_ref[...]
    image = raw_ref[...] + noise_ref[...] * rhs
    image_ref[...] = image
    values = rhs - THETA * image
    apply_kernel_matrix(col_pts, row_pts, values, out_ref, left, right, stack)


def product_scratch(outs, ins):
    return [
        pltpu.VMEM((outs, LANES), BF16),
        pltpu.VMEM((LANES, ins), BF16),
        pltpu.VMEM((ins // LANES, 256, 256), BF16),
    ]


def product_cost(outs, ins):
    return pl.CostEstimate(
        flops=2 * outs * ins * 512, bytes_accessed=8 * (outs + ins) * HALF, transcendentals=outs * ins
    )


def first_product(units, col_pts):
    ins, outs = units.shape[0] * 64, col_pts.shape[0] * 64
    return pl.pallas_call(
        first_product_kernel,
        in_specs=[VMEM] * 2,
        out_specs=VMEM,
        out_shape=jax.ShapeDtypeStruct((outs // 2, LANES), F32),
        scratch_shapes=product_scratch(outs, ins),
        cost_estimate=product_cost(outs, ins),
        name="first_product",
    )(units, col_pts)


def second_product(units, col_pts, raw, rhs, noise):
    outs, ins = units.shape[0] * 64, col_pts.shape[0] * 64
    return pl.pallas_call(
        second_product_kernel,
        in_specs=[VMEM] * 5,
        out_specs=[VMEM] * 2,
        out_shape=[
            jax.ShapeDtypeStruct((outs // 2, LANES), F32),
            jax.ShapeDtypeStruct((ins // 2, LANES), F32),
        ],
        scratch_shapes=product_scratch(outs, ins),
        cost_estimate=product_cost(outs, ins),
        name="second_product",
    )(units, col_pts, raw, rhs, noise)


def final_kernel(rhs_ref, packed_ref, image_ref, second_ref, sol_c_ref, res_c_ref, sol_ref, res_ref):
    low = lane_of((32, LANES)) < HALF

    def spread(ref, tile):
        pieces = []
        for part in range(2):
            rows = ref[tile * 64 + part * 32 : tile * 64 + part * 32 + 32]
            pieces += [jnp.where(low, rows, 0.0), jnp.where(low, 0.0, rows)]
        return jnp.concatenate(pieces, axis=0)

    def mixed(coefs, spreads):
        return lax.dot_general(
            coefs, spreads, (((1,), (1,)), ((), ())), precision=HIGH, preferred_element_type=F32
        )

    for tile in range(rhs_ref.shape[1] // LANES):
        cut = slice(tile * LANES, (tile + 1) * LANES)
        image = spread(image_ref, tile)
        sol_ref[:, cut] = mixed(
            sol_c_ref[...], jnp.concatenate([spread(packed_ref, tile), image], axis=1)
        )
        res_ref[:, cut] = rhs_ref[:, cut] - mixed(
            res_c_ref[...], jnp.concatenate([image, spread(second_ref, tile)], axis=1)
        )


def final_outputs(right_sides, rhs, image, second, sol_coefs, res_coefs):
    return pl.pallas_call(
        final_kernel,
        in_specs=[VMEM] * 6,
        out_specs=[VMEM] * 2,
        out_shape=[jax.ShapeDtypeStruct(right_sides.shape, F32)] * 2,
        name="final_outputs",
    )(right_sides, rhs, image, second, sol_coefs, res_coefs)


def exchanged(parts, axis):
    return lax.all_to_all(parts, axis, 0, 0, tiled=True)


def shared(value, axis):
    return exchanged(jnp.broadcast_to(value[None], (lax.axis_size(axis), *value.shape)), axis)


def solve_sym(matrix, target):
    lower = jnp.linalg.cholesky(0.5 * (matrix + matrix.T))
    return jax.scipy.linalg.cho_solve((lower, True), target)


def twice(coefs):
    zero = jnp.zeros_like(coefs)
    return jnp.block([[coefs, zero], [zero, coefs]])


def times(value, coefs):
    return jnp.dot(value, twice(coefs), precision=HIGH)


def side_by_side(first, second):
    return jnp.concatenate([first, second], axis=1)


def on_device(points, noise_level, right_sides):
    rows, cols = lax.axis_size("row"), lax.axis_size(COL)
    col_index = lax.axis_index(COL)[None].astype(jnp.int32)
    row_units, col_units = own_units(col_index, right_sides, points, rows, cols)
    units = exchanged(row_units, "row")
    col_pts = exchanged(col_units, COL)
    rhs, noise = packed_rows(right_sides, noise_level)

    part = first_product(units, col_pts).reshape(cols, 32, LANES)
    own = jnp.sum(exchanged(part, COL), axis=0)
    raw = shared(own, COL).reshape(-1, LANES)
    part, image = second_product(units, col_pts, raw, rhs, noise)
    part = part.reshape(rows, 32, LANES)

    grams = side_by_side(block_dot(rhs, rhs), block_dot(rhs, image))
    grams = jnp.sum(shared(grams, "row"), axis=0)
    gram, curv = grams[:, :HALF], grams[:, HALF:]
    own = jnp.sum(exchanged(part, "row"), axis=0)
    coef0 = solve_sym(curv, gram)
    residual = rhs - times(image, coef0)
    gram1 = block_dot(residual, residual)
    gram1 = side_by_side(gram1[:32], gram1[32:])
    gram1 = jnp.sum(shared(gram1, "row"), axis=0)
    gram1 = jnp.concatenate([gram1[:, :HALF], gram1[:, HALF:]], axis=0)
    raw = shared(own, COL).reshape(-1, LANES)
    dcoef = solve_sym(gram, gram1)
    second = raw + noise * (rhs - THETA * image)

    direction = residual + times(rhs, dcoef)
    scaled = coef0 / THETA
    image1 = times(image, jnp.eye(HALF, dtype=F32) - scaled + dcoef) + times(second, scaled)
    curv1 = block_dot(direction, image1)
    curv1 = side_by_side(curv1[:32], curv1[32:])
    curv1 = jnp.sum(shared(curv1, "row"), axis=0)
    curv1 = jnp.concatenate([curv1[:, :HALF], curv1[:, HALF:]], axis=0)
    coef1 = solve_sym(curv1, gram1)

    linear = coef0 + coef1 + jnp.dot(dcoef, coef1, precision=HIGH)
    square = jnp.dot(coef0, coef1, precision=HIGH)
    scaled = square / THETA
    doubled = lambda a, b: jnp.concatenate([a.T, a.T, b.T, b.T], axis=1)
    sol, res = final_outputs(
        right_sides, rhs, image, second, doubled(linear, -square), doubled(linear - scaled, scaled)
    )
    norms = jnp.sum(res * res, axis=1)[None, :]
    norms = jnp.sum(shared(side_by_side(norms, norms), "row"), axis=0)[0, :HALF]
    return sol, res, jnp.sqrt(norms / jnp.diagonal(gram))


def solution(mesh):
    torus = Mesh(
        mesh.devices.reshape(mesh.shape["row"], 4, 4, 2), ("row", "col_0", "col_1", "col_2")
    )
    return jax.shard_map(
        on_device,
        mesh=torus,
        in_specs=(P(None, ROW_COL), P("row"), P(None, "row")),
        out_specs=(P(None, "row"), P(None, "row"), P()),
        check_vma=False,
    )
```

```python
import jax
import jax.numpy as jnp
from jax import lax
from jax.experimental import pallas as pl
from jax.experimental.pallas import tpu as pltpu
from jax.sharding import Mesh
from jax.sharding import PartitionSpec as P

COL = ("col_0", "col_1", "col_2")
ROW_COL = ("row", "col_0", "col_1", "col_2")
HIGH = lax.Precision.HIGHEST
F32 = jnp.float32
BF16 = jnp.bfloat16
THETA = 0.5
LANES = 128
HALF = 64
VMEM = pl.BlockSpec(memory_space=pltpu.VMEM)
SMEM = pl.BlockSpec(memory_space=pltpu.SMEM)


def lane_of(shape):
    return lax.broadcasted_iota(jnp.int32, shape, len(shape) - 1)


def packed(turned):
    return jnp.concatenate([turned[:32], turned[32:64]], axis=1)


def own_kernel(col_ref, rhs_ref, pts_ref, row_out, col_out):
    turned = rhs_ref[...].T
    odd = lax.rem(col_ref[0], 2) == 1
    block = packed(jnp.where(odd, turned[HALF:], turned[:HALF]))
    pts = jnp.concatenate([pts_ref[...], pts_ref[...]], axis=1)
    unit = jnp.concatenate([block, pts], axis=0)
    for place in range(row_out.shape[0]):
        row_out[place] = unit
    for place in range(col_out.shape[0]):
        col_out[place] = pts


def own_units(col_index, right_sides, points, rows, cols):
    return pl.pallas_call(
        own_kernel,
        grid_spec=pltpu.PrefetchScalarGridSpec(
            num_scalar_prefetch=1,
            grid=(1,),
            in_specs=[
                pl.BlockSpec((HALF, LANES), lambda i, c: (0, c[0] // 2)),
                pl.BlockSpec((8, HALF), lambda i, c: (0, 0)),
            ],
            out_specs=[
                pl.BlockSpec((rows, 40, LANES), lambda i, c: (0, 0, 0)),
                pl.BlockSpec((cols, 8, LANES), lambda i, c: (0, 0, 0)),
            ],
        ),
        out_shape=[
            jax.ShapeDtypeStruct((rows, 40, LANES), F32),
            jax.ShapeDtypeStruct((cols, 8, LANES), F32),
        ],
        name="own_units",
    )(col_index, right_sides, points)


def packed_kernel(rhs_ref, noise_ref, packed_out, noise_out):
    low = lane_of((32, LANES)) < HALF
    for tile in range(rhs_ref.shape[1] // LANES):
        turned = rhs_ref[:, tile * LANES : (tile + 1) * LANES].T
        noise = noise_ref[:, tile * LANES : (tile + 1) * LANES]
        noise = jnp.broadcast_to(noise, (LANES, LANES)).T
        for part in range(2):
            rows = slice(tile * 64 + part * 32, tile * 64 + part * 32 + 32)
            packed_out[rows] = packed(turned[part * 64 : part * 64 + 64])
            noise_out[rows] = jnp.where(
                low, noise[part * 64 : part * 64 + 32], noise[part * 64 + 32 : part * 64 + 64]
            )


def packed_rows(right_sides, noise_level):
    rows = right_sides.shape[1] // 2
    return pl.pallas_call(
        packed_kernel,
        in_specs=[VMEM] * 2,
        out_specs=[VMEM] * 2,
        out_shape=[jax.ShapeDtypeStruct((rows, LANES), F32)] * 2,
        cost_estimate=pl.CostEstimate(
            flops=4 * 10**9, bytes_accessed=3 * 4 * rows * LANES, transcendentals=0
        ),
        name="packed_rows",
    )(right_sides, noise_level[None, :])


def ordered(units):
    place = lane_of((8, LANES)) // 32
    pieces = []
    for h in range(2):
        for start in range(0, len(units), 4):
            piece = None
            for q in range(4):
                unit = units[start + q]
                if (q - h) % 2:
                    unit = pltpu.roll(unit, 32, 1)
                piece = unit if piece is None else jnp.where(place == q, unit, piece)
            pieces.append(piece)
    return jnp.concatenate(pieces, axis=1)


def rounded(value):
    return value.astype(BF16).astype(F32)


def three_parts(value):
    first = rounded(value)
    rest = value - first
    second = rounded(rest)
    return first, second, rest - second


def augmented(pts, as_rows):
    x1, x2, x3 = three_parts(pts)
    half_sq = -0.5 * jnp.sum(pts * pts, axis=0, keepdims=True)
    s1, s2, s3 = three_parts(half_sq)
    sub = lax.broadcasted_iota(jnp.int32, pts.shape, 0)
    squares = jnp.where(sub == 0, s1, jnp.where(sub == 1, s2, jnp.where(sub == 2, s3, 0.0)))
    ones = jnp.where(sub < 3, 1.0, 0.0)
    zeros = jnp.zeros_like(pts)
    if as_rows:
        blocks = [x1, x1, x2, x2, x1, x3, x2, x3, squares, ones]
    else:
        blocks = [x1, x2, x1, x2, x3, x1, x3, x2, ones, squares]
    return jnp.concatenate(blocks + [zeros] * 6, axis=0)


def apply_kernel_matrix(out_pts, in_pts, values, result, left, right, stack):
    outs = left.shape[0]
    ins = right.shape[1]
    tile = min(256, outs // 2)
    for start in range(0, outs, LANES):
        piece = augmented(out_pts[:, start : start + LANES], True)
        left[start : start + LANES] = piece.T.astype(BF16)
    for start in range(0, ins, 256):
        right[:, start : start + 256] = augmented(in_pts[:, start : start + 256], False).astype(BF16)
    groups = ins // 256
    low = lane_of((LANES, LANES)) < HALF
    for group in range(groups):
        rows = values[group * LANES : (group + 1) * LANES]
        turned = pltpu.roll(rows, HALF, 1)
        for h in range(2):
            top = jnp.where(low, turned if h else rows, 0.0)
            bottom = jnp.where(low, 0.0, rows if h else turned)
            both = jnp.concatenate([top, bottom], axis=0)
            high = both.astype(BF16)
            rest = (both - high.astype(F32)).astype(BF16)
            stack[h * groups + group, :, :LANES] = high
            stack[h * groups + group, :, LANES:] = rest
    result[...] = jnp.zeros_like(result)
    pairs = ins // 256

    def step(index, carry):
        at = pl.multiple_of(lax.div(index, pairs) * tile, tile)
        pair = lax.rem(index, pairs)
        columns = right[:, pl.ds(pl.multiple_of(pair * 256, 256), 256)]
        highs, lows = [], []
        for h in range(2):
            lines = left[pl.ds(h * (outs // 2) + at, tile)]
            kernel = jnp.exp(jnp.dot(lines, columns, preferred_element_type=F32))
            high = kernel.astype(BF16)
            highs.append(high)
            lows.append((kernel - high.astype(F32)).astype(BF16))
        total = result[pl.ds(at, tile)]
        for a in range(2):
            weights = stack[pair * 2 + a]
            cut = slice(a * LANES, (a + 1) * LANES)
            high = jnp.concatenate([highs[0][:, cut], highs[1][:, cut]], axis=1)
            rest = jnp.concatenate([lows[0][:, cut], lows[1][:, cut]], axis=1)
            both = jnp.dot(high, weights, preferred_element_type=F32)
            total = total + both[:, :LANES] + both[:, LANES:]
            total = total + jnp.dot(rest, weights[:, :LANES], preferred_element_type=F32)
        result[pl.ds(at, tile)] = total
        return carry

    lax.fori_loop(0, (outs // 2 // tile) * pairs, step, 0)


def first_product_kernel(unit_ref, col_ref, out_ref, left, right, stack):
    col_pts = ordered([unit_ref[i, 32:] for i in range(unit_ref.shape[0])])
    row_pts = ordered([col_ref[i] for i in range(col_ref.shape[0])])
    values = jnp.concatenate([unit_ref[i, :32] for i in range(unit_ref.shape[0])], axis=0)
    apply_kernel_matrix(row_pts, col_pts, values, out_ref, left, right, stack)


def second_product_kernel(
    place_ref, unit_ref, col_ref, raw_ref, rhs_ref, noise_ref, out_ref, image_ref, left, right, stack, result, grams
):
    col_pts = ordered([unit_ref[i, 32:] for i in range(unit_ref.shape[0])])
    row_pts = ordered([col_ref[i] for i in range(col_ref.shape[0])])
    rhs = rhs_ref[...]
    image = raw_ref[...] + noise_ref[...] * rhs
    image_ref[...] = image
    values = rhs - THETA * image
    apply_kernel_matrix(col_pts, row_pts, values, result, left, right, stack)
    both = jnp.concatenate([rhs, image], axis=1)
    gram = transposed_dot(both, both)
    grams[0:32] = folded(gram[:LANES, :LANES])
    grams[32:64] = folded(gram[:LANES, LANES:])
    grams[64:96] = folded(gram[LANES:, LANES:])
    lines = [grams[pl.ds(32 * m + place_ref[0], 1)] for m in range(3)]
    tail = jnp.concatenate(lines + [jnp.zeros((5, LANES), F32)], axis=0)
    for place in range(out_ref.shape[0]):
        out_ref[place, :32] = result[place * 32 : place * 32 + 32]
        out_ref[place, 32:] = tail


def product_scratch(outs, ins):
    return [
        pltpu.VMEM((outs, LANES), BF16),
        pltpu.VMEM((LANES, ins), BF16),
        pltpu.VMEM((ins // LANES, 256, 256), BF16),
    ]


def product_cost(outs, ins):
    return pl.CostEstimate(
        flops=2 * outs * ins * 512, bytes_accessed=8 * (outs + ins) * HALF, transcendentals=outs * ins
    )


def first_product(units, col_pts):
    ins, outs = units.shape[0] * 64, col_pts.shape[0] * 64
    return pl.pallas_call(
        first_product_kernel,
        in_specs=[VMEM] * 2,
        out_specs=VMEM,
        out_shape=jax.ShapeDtypeStruct((outs // 2, LANES), F32),
        scratch_shapes=product_scratch(outs, ins),
        cost_estimate=product_cost(outs, ins),
        name="first_product",
    )(units, col_pts)


def second_product(place, units, col_pts, raw, rhs, noise):
    outs, ins = units.shape[0] * 64, col_pts.shape[0] * 64
    return pl.pallas_call(
        second_product_kernel,
        in_specs=[SMEM] + [VMEM] * 5,
        out_specs=[VMEM] * 2,
        out_shape=[
            jax.ShapeDtypeStruct((units.shape[0], 40, LANES), F32),
            jax.ShapeDtypeStruct((ins // 2, LANES), F32),
        ],
        scratch_shapes=product_scratch(outs, ins)
        + [pltpu.VMEM((outs // 2, LANES), F32), pltpu.VMEM((96, LANES), F32)],
        cost_estimate=product_cost(outs, ins),
        name="second_product",
    )(place, units, col_pts, raw, rhs, noise)


def transposed_dot(first, second):
    return lax.dot_general(
        first, second, (((0,), (0,)), ((), ())), precision=HIGH, preferred_element_type=F32
    )


def folded(gram):
    total = gram[:HALF, :HALF] + gram[HALF:, HALF:]
    return jnp.concatenate([total[:32], total[32:]], axis=1)


def unfolded(lines):
    return jnp.concatenate([lines[:, :HALF], lines[:, HALF:]], axis=0)


def small_dot(first, second):
    return jnp.dot(first, second, precision=HIGH, preferred_element_type=F32)


def twice(coefs):
    zero = jnp.zeros_like(coefs)
    return jnp.concatenate(
        [jnp.concatenate([coefs, zero], axis=1), jnp.concatenate([zero, coefs], axis=1)], axis=0
    )


def line(tile, index):
    return jnp.broadcast_to(tile[index : index + 1], tile.shape)


def solve_sym(matrix, target):
    joined = jnp.concatenate([0.5 * (matrix + matrix.T), target], axis=1)
    tiles = tuple(joined[8 * t : 8 * t + 8] for t in range(8))
    sub = lax.broadcasted_iota(jnp.int32, (8, LANES), 0)

    def step(group, tiles):
        tiles = list(tiles)
        for quad in range(2):
            columns = []
            for j in range(4):
                lane = jnp.full((8, LANES), group * 8 + quad * 4 + j, jnp.int32)
                columns.append([jnp.take_along_axis(tile, lane, axis=1) for tile in tiles])
            for j in range(4):
                at = quad * 4 + j
                here = sub == at
                inverse = 1.0 / line(columns[j][0], at)
                row = line(tiles[0], at) * inverse
                for t in range(8):
                    new = tiles[t] - columns[j][t] * row
                    tiles[t] = jnp.where(here, row, new) if t == 0 else new
                for later in range(j + 1, 4):
                    ratio = line(columns[later][0], at) * inverse
                    for t in range(8):
                        new = columns[later][t] - columns[j][t] * ratio
                        columns[later][t] = jnp.where(here, ratio, new) if t == 0 else new
        return tuple(tiles[1:] + tiles[:1])

    tiles = lax.fori_loop(0, 8, step, tiles)
    return jnp.concatenate(tiles, axis=0)[:, HALF:]


def middle_kernel(core_ref, unit_ref, rhs_ref, image_ref, noise_ref, share_ref, second_ref, coef_ref, lines):
    for place in range(unit_ref.shape[0]):
        tail = unit_ref[place, 32:]
        for m in range(3):
            lines[32 * m + place : 32 * m + place + 1] = tail[m : m + 1]
    gram, curv, square = (unfolded(lines[32 * m : 32 * m + 32]) for m in range(3))
    coef0 = solve_sym(curv, gram)
    cross = small_dot(curv, coef0)
    gram1 = gram - cross - cross.T + small_dot(coef0.T, small_dot(square, coef0))
    dcoef = solve_sym(gram, gram1)
    rhs, image = rhs_ref[...], image_ref[...]
    raw = jnp.concatenate([unit_ref[i, :32] for i in range(unit_ref.shape[0])], axis=0)
    second = raw + noise_ref[...] * (rhs - THETA * image)
    second_ref[...] = second
    residual = rhs - small_dot(image, twice(coef0))
    direction = residual + small_dot(rhs, twice(dcoef))
    scaled = coef0 * (1.0 / THETA)
    eye = (
        lax.broadcasted_iota(jnp.int32, (HALF, HALF), 0) == lax.broadcasted_iota(jnp.int32, (HALF, HALF), 1)
    ).astype(F32)
    image1 = small_dot(
        jnp.concatenate([image, second], axis=1),
        jnp.concatenate([twice(eye - scaled + dcoef), twice(scaled)], axis=0),
    )
    crossed = transposed_dot(jnp.concatenate([direction, image1], axis=1), image1)
    lines[0:32] = folded(crossed[:LANES])
    lines[32:64] = folded(crossed[LANES:])
    lines[64:96] = folded(transposed_dot(residual, residual))
    start = pl.multiple_of(core_ref[0] * 16, 16)
    part = jnp.concatenate([lines[pl.ds(32 * m + start, 16)] for m in range(3)], axis=0)
    for place in range(share_ref.shape[0]):
        share_ref[place] = part
    coef_ref[0:64] = jnp.concatenate([coef0, dcoef], axis=1)
    coef_ref[64:128] = jnp.concatenate([gram, eye], axis=1)


def middle(core, units, rhs, image, noise, rows):
    return pl.pallas_call(
        middle_kernel,
        in_specs=[SMEM] + [VMEM] * 4,
        out_specs=[VMEM] * 3,
        out_shape=[
            jax.ShapeDtypeStruct((rows, 48, LANES), F32),
            jax.ShapeDtypeStruct(rhs.shape, F32),
            jax.ShapeDtypeStruct((128, LANES), F32),
        ],
        scratch_shapes=[pltpu.VMEM((96, LANES), F32)],
        name="middle",
    )(core, units, rhs, image, noise)


def final_kernel(lines_ref, coef_ref, rhs_ref, packed_ref, image_ref, second_ref, sol_ref, res_ref, norm_ref):
    low = lane_of((32, LANES)) < HALF
    curv1, square, gram1 = (
        unfolded(jnp.concatenate([lines_ref[half, 16 * m : 16 * m + 16] for half in range(2)], axis=0))
        for m in range(3)
    )
    coef0, dcoef = coef_ref[0:64, :HALF], coef_ref[0:64, HALF:]
    gram, eye = coef_ref[64:128, :HALF], coef_ref[64:128, HALF:]
    coef1 = solve_sym(curv1, gram1)
    cross = small_dot(curv1, coef1)
    gram2 = gram1 - cross - cross.T + small_dot(coef1.T, small_dot(square, coef1))
    norms = jnp.sum(eye * gram2, axis=0, keepdims=True) / jnp.sum(eye * gram, axis=0, keepdims=True)
    norm_ref[...] = jnp.sqrt(jnp.maximum(norms, 0.0))
    linear = coef0 + coef1 + small_dot(dcoef, coef1)
    quadratic = small_dot(coef0, coef1)
    scaled = quadratic * (1.0 / THETA)

    def doubled(first, second):
        first, second = first.T, second.T
        return jnp.concatenate([first, first, second, second], axis=1)

    sol_c = doubled(linear, -quadratic)
    res_c = doubled(linear - scaled, scaled)

    def spread(ref, tile):
        pieces = []
        for part in range(2):
            rows = ref[tile * 64 + part * 32 : tile * 64 + part * 32 + 32]
            pieces += [jnp.where(low, rows, 0.0), jnp.where(low, 0.0, rows)]
        return jnp.concatenate(pieces, axis=0)

    def mixed(coefs, spreads):
        return lax.dot_general(
            coefs, spreads, (((1,), (1,)), ((), ())), precision=HIGH, preferred_element_type=F32
        )

    for tile in range(rhs_ref.shape[1] // LANES):
        cut = slice(tile * LANES, (tile + 1) * LANES)
        image = spread(image_ref, tile)
        sol_ref[:, cut] = mixed(sol_c, jnp.concatenate([spread(packed_ref, tile), image], axis=1))
        res_ref[:, cut] = rhs_ref[:, cut] - mixed(
            res_c, jnp.concatenate([image, spread(second_ref, tile)], axis=1)
        )


def final_outputs(lines, coefs, right_sides, rhs, image, second):
    return pl.pallas_call(
        final_kernel,
        in_specs=[VMEM] * 6,
        out_specs=[VMEM] * 3,
        out_shape=[jax.ShapeDtypeStruct(right_sides.shape, F32)] * 2
        + [jax.ShapeDtypeStruct((1, HALF), F32)],
        name="final_outputs",
    )(lines, coefs, right_sides, rhs, image, second)


def exchanged(parts, axis):
    return lax.all_to_all(parts, axis, 0, 0, tiled=True)


def shared(value, axis):
    return exchanged(jnp.broadcast_to(value[None], (lax.axis_size(axis), *value.shape)), axis)


def on_device(points, noise_level, right_sides):
    rows, cols = lax.axis_size("row"), lax.axis_size(COL)
    col_index = lax.axis_index(COL)[None].astype(jnp.int32)
    row_units, col_units = own_units(col_index, right_sides, points, rows, cols)
    units = exchanged(row_units, "row")
    col_pts = exchanged(col_units, COL)
    rhs, noise = packed_rows(right_sides, noise_level)

    part = first_product(units, col_pts).reshape(cols, 32, LANES)
    own = jnp.sum(exchanged(part, COL), axis=0)
    raw = shared(own, COL).reshape(-1, LANES)
    part, image = second_product(col_index, units, col_pts, raw, rhs, noise)
    own = jnp.sum(exchanged(part, "row"), axis=0)
    core = lax.axis_index(COL[-1])[None].astype(jnp.int32)
    share, second, coefs = middle(core, shared(own, COL), rhs, image, noise, rows)
    lines = lax.all_gather(jnp.sum(exchanged(share, "row"), axis=0), COL[-1])
    sol, res, norms = final_outputs(lines, coefs, right_sides, rhs, image, second)
    return sol, res, norms[0]


def solution(mesh):
    torus = Mesh(
        mesh.devices.reshape(mesh.shape["row"], 4, 4, 2), ("row", "col_0", "col_1", "col_2")
    )
    return jax.shard_map(
        on_device,
        mesh=torus,
        in_specs=(P(None, ROW_COL), P("row"), P(None, "row")),
        out_specs=(P(None, "row"), P(None, "row"), P()),
        check_vma=False,
    )
```

```python
import jax
import jax.numpy as jnp
from jax import lax
from jax.experimental import pallas as pl
from jax.experimental.pallas import tpu as pltpu
from jax.sharding import Mesh
from jax.sharding import PartitionSpec as P

COL = ("col_0", "col_1", "col_2")
ROW_COL = ("row", "col_0", "col_1", "col_2")
HIGH = lax.Precision.HIGHEST
F32 = jnp.float32
BF16 = jnp.bfloat16
THETA = 0.5
LANES = 128
HALF = 64
VMEM = pl.BlockSpec(memory_space=pltpu.VMEM)
SMEM = pl.BlockSpec(memory_space=pltpu.SMEM)


def lane_of(shape):
    return lax.broadcasted_iota(jnp.int32, shape, len(shape) - 1)


def packed(turned):
    return jnp.concatenate([turned[:32], turned[32:64]], axis=1)


def own_kernel(pts_ref, row_out, col_out):
    unit = jnp.concatenate([pts_ref[:4], pts_ref[4:]], axis=1)
    for place in range(row_out.shape[0]):
        row_out[place] = unit
    for place in range(col_out.shape[0]):
        col_out[place] = unit


def own_units(points, rows, cols):
    return pl.pallas_call(
        own_kernel,
        in_specs=[VMEM],
        out_specs=[VMEM] * 2,
        out_shape=[
            jax.ShapeDtypeStruct((rows, 4, LANES), F32),
            jax.ShapeDtypeStruct((cols, 4, LANES), F32),
        ],
        name="own_units",
    )(points)


def packed_kernel(rhs_ref, noise_ref, packed_out, noise_out):
    low = lane_of((32, LANES)) < HALF
    for tile in range(rhs_ref.shape[1] // LANES):
        turned = rhs_ref[:, tile * LANES : (tile + 1) * LANES].T
        noise = noise_ref[:, tile * LANES : (tile + 1) * LANES]
        noise = jnp.broadcast_to(noise, (LANES, LANES)).T
        for part in range(2):
            rows = slice(tile * 64 + part * 32, tile * 64 + part * 32 + 32)
            packed_out[rows] = packed(turned[part * 64 : part * 64 + 64])
            noise_out[rows] = jnp.where(
                low, noise[part * 64 : part * 64 + 32], noise[part * 64 + 32 : part * 64 + 64]
            )


def packed_rows(right_sides, noise_level):
    rows = right_sides.shape[1] // 2
    return pl.pallas_call(
        packed_kernel,
        in_specs=[VMEM] * 2,
        out_specs=[VMEM] * 2,
        out_shape=[jax.ShapeDtypeStruct((rows, LANES), F32)] * 2,
        cost_estimate=pl.CostEstimate(
            flops=4 * 10**9, bytes_accessed=3 * 4 * rows * LANES, transcendentals=0
        ),
        name="packed_rows",
    )(right_sides, noise_level[None, :])


def ordered(ref):
    place = lane_of((8, LANES)) // 32
    low = lane_of((4, LANES)) < HALF
    units = []
    for index in range(ref.shape[0]):
        unit = ref[index]
        turned = pltpu.roll(unit, HALF, 1)
        units.append(
            jnp.concatenate([jnp.where(low, unit, turned), jnp.where(low, turned, unit)], axis=0)
        )
    pieces = []
    for h in range(2):
        for start in range(0, len(units), 4):
            piece = None
            for q in range(4):
                unit = units[start + q]
                if (q - h) % 2:
                    unit = pltpu.roll(unit, 32, 1)
                piece = unit if piece is None else jnp.where(place == q, unit, piece)
            pieces.append(piece)
    return jnp.concatenate(pieces, axis=1)


def rounded(value):
    return value.astype(BF16).astype(F32)


def three_parts(value):
    first = rounded(value)
    rest = value - first
    second = rounded(rest)
    return first, second, rest - second


def augmented(pts, as_rows):
    x1, x2, x3 = three_parts(pts)
    half_sq = -0.5 * jnp.sum(pts * pts, axis=0, keepdims=True)
    s1, s2, s3 = three_parts(half_sq)
    sub = lax.broadcasted_iota(jnp.int32, pts.shape, 0)
    squares = jnp.where(sub == 0, s1, jnp.where(sub == 1, s2, jnp.where(sub == 2, s3, 0.0)))
    ones = jnp.where(sub < 3, 1.0, 0.0)
    zeros = jnp.zeros_like(pts)
    if as_rows:
        blocks = [x1, x1, x2, x2, x1, x3, x2, x3, squares, ones]
    else:
        blocks = [x1, x2, x1, x2, x3, x1, x3, x2, ones, squares]
    return jnp.concatenate(blocks + [zeros] * 6, axis=0)


def apply_kernel_matrix(out_pts, in_pts, values, result, left, right, stack):
    outs = left.shape[0]
    ins = right.shape[1]
    tile = min(256, outs // 2)
    for start in range(0, outs, LANES):
        piece = augmented(out_pts[:, start : start + LANES], True)
        left[start : start + LANES] = piece.T.astype(BF16)
    for start in range(0, ins, 256):
        right[:, start : start + 256] = augmented(in_pts[:, start : start + 256], False).astype(BF16)
    groups = ins // 256
    low = lane_of((LANES, LANES)) < HALF
    for group in range(groups):
        rows = values[group * LANES : (group + 1) * LANES]
        turned = pltpu.roll(rows, HALF, 1)
        for h in range(2):
            top = jnp.where(low, turned if h else rows, 0.0)
            bottom = jnp.where(low, 0.0, rows if h else turned)
            both = jnp.concatenate([top, bottom], axis=0)
            high = both.astype(BF16)
            rest = (both - high.astype(F32)).astype(BF16)
            stack[h * groups + group, :, :LANES] = high
            stack[h * groups + group, :, LANES:] = rest
    result[...] = jnp.zeros_like(result)
    pairs = ins // 256

    def step(index, carry):
        at = pl.multiple_of(lax.div(index, pairs) * tile, tile)
        pair = lax.rem(index, pairs)
        columns = right[:, pl.ds(pl.multiple_of(pair * 256, 256), 256)]
        highs, lows = [], []
        for h in range(2):
            lines = left[pl.ds(h * (outs // 2) + at, tile)]
            kernel = jnp.exp(jnp.dot(lines, columns, preferred_element_type=F32))
            high = kernel.astype(BF16)
            highs.append(high)
            lows.append((kernel - high.astype(F32)).astype(BF16))
        total = result[pl.ds(at, tile)]
        for a in range(2):
            weights = stack[pair * 2 + a]
            cut = slice(a * LANES, (a + 1) * LANES)
            high = jnp.concatenate([highs[0][:, cut], highs[1][:, cut]], axis=1)
            rest = jnp.concatenate([lows[0][:, cut], lows[1][:, cut]], axis=1)
            both = jnp.dot(high, weights, preferred_element_type=F32)
            total = total + both[:, :LANES] + both[:, LANES:]
            total = total + jnp.dot(rest, weights[:, :LANES], preferred_element_type=F32)
        result[pl.ds(at, tile)] = total
        return carry

    lax.fori_loop(0, (outs // 2 // tile) * pairs, step, 0)


def first_product_kernel(row_ref, col_ref, rhs_ref, out_ref, left, right, stack, result):
    apply_kernel_matrix(ordered(row_ref), ordered(col_ref), rhs_ref[...], result, left, right, stack)
    for place in range(out_ref.shape[0]):
        out_ref[place] = result[place * 32 : place * 32 + 32]


def second_product_kernel(
    place_ref, row_ref, col_ref, raw_ref, rhs_ref, noise_ref, out_ref, image_ref, left, right, stack, result, grams
):
    rhs = rhs_ref[...]
    image = raw_ref[...] + noise_ref[...] * rhs
    image_ref[...] = image
    values = rhs - THETA * image
    apply_kernel_matrix(ordered(row_ref), ordered(col_ref), values, result, left, right, stack)
    both = jnp.concatenate([rhs, image], axis=1)
    gram = transposed_dot(both, both)
    grams[0:32] = folded(summed_halves(gram[:LANES, :LANES]))
    grams[32:64] = folded(summed_halves(gram[:LANES, LANES:]))
    grams[64:96] = folded(summed_halves(gram[LANES:, LANES:]))
    lines = [grams[pl.ds(32 * m + place_ref[0], 1)] for m in range(3)]
    tail = jnp.concatenate(lines + [jnp.zeros((5, LANES), F32)], axis=0)
    for place in range(out_ref.shape[0]):
        out_ref[place, :32] = result[place * 32 : place * 32 + 32]
        out_ref[place, 32:] = tail


def product_scratch(outs, ins):
    return [
        pltpu.VMEM((outs, LANES), BF16),
        pltpu.VMEM((LANES, ins), BF16),
        pltpu.VMEM((ins // LANES, 256, 256), BF16),
        pltpu.VMEM((outs // 2, LANES), F32),
    ]


def product_cost(outs, ins):
    return pl.CostEstimate(
        flops=2 * outs * ins * 512, bytes_accessed=8 * (outs + ins) * HALF, transcendentals=outs * ins
    )


def first_product(row_pts, col_pts, rhs):
    outs, ins = row_pts.shape[0] * 64, col_pts.shape[0] * 64
    return pl.pallas_call(
        first_product_kernel,
        in_specs=[VMEM] * 3,
        out_specs=VMEM,
        out_shape=jax.ShapeDtypeStruct((row_pts.shape[0], 32, LANES), F32),
        scratch_shapes=product_scratch(outs, ins),
        cost_estimate=product_cost(outs, ins),
        name="first_product",
    )(row_pts, col_pts, rhs)


def second_product(place, row_pts, col_pts, raw, rhs, noise):
    outs, ins = row_pts.shape[0] * 64, col_pts.shape[0] * 64
    return pl.pallas_call(
        second_product_kernel,
        in_specs=[SMEM] + [VMEM] * 5,
        out_specs=[VMEM] * 2,
        out_shape=[
            jax.ShapeDtypeStruct((row_pts.shape[0], 40, LANES), F32),
            jax.ShapeDtypeStruct((ins // 2, LANES), F32),
        ],
        scratch_shapes=product_scratch(outs, ins) + [pltpu.VMEM((96, LANES), F32)],
        cost_estimate=product_cost(outs, ins),
        name="second_product",
    )(place, row_pts, col_pts, raw, rhs, noise)


def transposed_dot(first, second):
    return lax.dot_general(
        first, second, (((0,), (0,)), ((), ())), precision=HIGH, preferred_element_type=F32
    )


def summed_halves(gram):
    return gram[:HALF, :HALF] + gram[HALF:, HALF:]


def folded(square):
    return jnp.concatenate([square[:32], square[32:]], axis=1)


def unfolded(lines):
    return jnp.concatenate([lines[:, :HALF], lines[:, HALF:]], axis=0)


def row_and_column():
    shape = (HALF, HALF)
    return lax.broadcasted_iota(jnp.int32, shape, 0), lax.broadcasted_iota(jnp.int32, shape, 1)


def squares_of(first, second, third):
    row, column = row_and_column()
    diagonal = jnp.sum(jnp.where(row == column, second, 0.0), axis=0, keepdims=True)
    under = jnp.where(row == HALF - 1, diagonal, jnp.where(row == HALF - 2, diagonal[:, HALF - 1 :], 0.0))
    return jnp.where(column >= row, first, second), jnp.where(column >= row, third, under)


def matrices_of(upper, lower):
    row, column = row_and_column()
    turned, beneath = upper.T, lower.T
    diagonal = jnp.where(column == HALF - 1, lower[HALF - 2 : HALF - 1, :1], lower[HALF - 1 :])
    first = jnp.where(column >= row, upper, turned)
    second = jnp.where(column == row, diagonal, jnp.where(column < row, upper, turned))
    return first, second, jnp.where(column >= row, lower, beneath)


def small_dot(first, second):
    return jnp.dot(first, second, precision=HIGH, preferred_element_type=F32)


def twice(coefs):
    zero = jnp.zeros_like(coefs)
    return jnp.concatenate(
        [jnp.concatenate([coefs, zero], axis=1), jnp.concatenate([zero, coefs], axis=1)], axis=0
    )


def line(tile, index):
    return jnp.broadcast_to(tile[index : index + 1], tile.shape)


def solve_sym(matrix, target):
    joined = jnp.concatenate([0.5 * (matrix + matrix.T), target], axis=1)
    tiles = tuple(joined[8 * t : 8 * t + 8] for t in range(8))
    sub = lax.broadcasted_iota(jnp.int32, (8, LANES), 0)

    def step(group, tiles):
        tiles = list(tiles)
        for quad in range(2):
            columns = []
            for j in range(4):
                lane = jnp.full((8, LANES), group * 8 + quad * 4 + j, jnp.int32)
                columns.append([jnp.take_along_axis(tile, lane, axis=1) for tile in tiles])
            for j in range(4):
                at = quad * 4 + j
                here = sub == at
                inverse = 1.0 / line(columns[j][0], at)
                row = line(tiles[0], at) * inverse
                for t in range(8):
                    new = tiles[t] - columns[j][t] * row
                    tiles[t] = jnp.where(here, row, new) if t == 0 else new
                for later in range(j + 1, 4):
                    ratio = line(columns[later][0], at) * inverse
                    for t in range(8):
                        new = columns[later][t] - columns[j][t] * ratio
                        columns[later][t] = jnp.where(here, ratio, new) if t == 0 else new
        return tuple(tiles[1:] + tiles[:1])

    tiles = lax.fori_loop(0, 8, step, tiles)
    return jnp.concatenate(tiles, axis=0)[:, HALF:]


def middle_kernel(core_ref, unit_ref, rhs_ref, image_ref, noise_ref, share_ref, second_ref, coef_ref, lines):
    for place in range(unit_ref.shape[0]):
        tail = unit_ref[place, 32:]
        for m in range(3):
            lines[32 * m + place : 32 * m + place + 1] = tail[m : m + 1]
    gram, curv, square = (unfolded(lines[32 * m : 32 * m + 32]) for m in range(3))
    coef0 = solve_sym(curv, gram)
    cross = small_dot(curv, coef0)
    gram1 = gram - cross - cross.T + small_dot(coef0.T, small_dot(square, coef0))
    dcoef = solve_sym(gram, gram1)
    rhs, image = rhs_ref[...], image_ref[...]
    raw = jnp.concatenate([unit_ref[i, :32] for i in range(unit_ref.shape[0])], axis=0)
    second = raw + noise_ref[...] * (rhs - THETA * image)
    second_ref[...] = second
    residual = rhs - small_dot(image, twice(coef0))
    direction = residual + small_dot(rhs, twice(dcoef))
    scaled = coef0 * (1.0 / THETA)
    eye = (
        lax.broadcasted_iota(jnp.int32, (HALF, HALF), 0) == lax.broadcasted_iota(jnp.int32, (HALF, HALF), 1)
    ).astype(F32)
    image1 = small_dot(
        jnp.concatenate([image, second], axis=1),
        jnp.concatenate([twice(eye - scaled + dcoef), twice(scaled)], axis=0),
    )
    crossed = transposed_dot(jnp.concatenate([direction, image1], axis=1), image1)
    curv1 = summed_halves(crossed[:LANES])
    upper, lower = squares_of(
        0.5 * (curv1 + curv1.T),
        summed_halves(transposed_dot(residual, residual)),
        summed_halves(crossed[LANES:]),
    )
    lines[0:32] = folded(upper)
    lines[32:64] = folded(lower)
    start = pl.multiple_of(core_ref[0] * 16, 16)
    part = jnp.concatenate([lines[pl.ds(32 * m + start, 16)] for m in range(2)], axis=0)
    for place in range(share_ref.shape[0]):
        share_ref[place] = part
    coef_ref[0:64] = jnp.concatenate([coef0, dcoef], axis=1)
    coef_ref[64:128] = jnp.concatenate([gram, eye], axis=1)


def middle(core, units, rhs, image, noise, rows):
    return pl.pallas_call(
        middle_kernel,
        in_specs=[SMEM] + [VMEM] * 4,
        out_specs=[VMEM] * 3,
        out_shape=[
            jax.ShapeDtypeStruct((rows, 32, LANES), F32),
            jax.ShapeDtypeStruct(rhs.shape, F32),
            jax.ShapeDtypeStruct((128, LANES), F32),
        ],
        scratch_shapes=[pltpu.VMEM((96, LANES), F32)],
        name="middle",
    )(core, units, rhs, image, noise)


def final_kernel(lines_ref, coef_ref, rhs_ref, packed_ref, image_ref, second_ref, sol_ref, res_ref, norm_ref):
    low = lane_of((32, LANES)) < HALF
    upper, lower = (
        unfolded(jnp.concatenate([lines_ref[half, 16 * m : 16 * m + 16] for half in range(2)], axis=0))
        for m in range(2)
    )
    curv1, gram1, square = matrices_of(upper, lower)
    coef0, dcoef = coef_ref[0:64, :HALF], coef_ref[0:64, HALF:]
    gram, eye = coef_ref[64:128, :HALF], coef_ref[64:128, HALF:]
    coef1 = solve_sym(curv1, gram1)
    cross = small_dot(curv1, coef1)
    gram2 = gram1 - cross - cross.T + small_dot(coef1.T, small_dot(square, coef1))
    norms = jnp.sum(eye * gram2, axis=0, keepdims=True) / jnp.sum(eye * gram, axis=0, keepdims=True)
    norm_ref[...] = jnp.sqrt(jnp.maximum(norms, 0.0))
    linear = coef0 + coef1 + small_dot(dcoef, coef1)
    quadratic = small_dot(coef0, coef1)
    scaled = quadratic * (1.0 / THETA)

    def doubled(first, second):
        first, second = first.T, second.T
        return jnp.concatenate([first, first, second, second], axis=1)

    sol_c = doubled(linear, -quadratic)
    res_c = doubled(linear - scaled, scaled)

    def spread(ref, tile):
        pieces = []
        for part in range(2):
            rows = ref[tile * 64 + part * 32 : tile * 64 + part * 32 + 32]
            pieces += [jnp.where(low, rows, 0.0), jnp.where(low, 0.0, rows)]
        return jnp.concatenate(pieces, axis=0)

    def mixed(coefs, spreads):
        return lax.dot_general(
            coefs, spreads, (((1,), (1,)), ((), ())), precision=HIGH, preferred_element_type=F32
        )

    for tile in range(rhs_ref.shape[1] // LANES):
        cut = slice(tile * LANES, (tile + 1) * LANES)
        image = spread(image_ref, tile)
        sol_ref[:, cut] = mixed(sol_c, jnp.concatenate([spread(packed_ref, tile), image], axis=1))
        res_ref[:, cut] = rhs_ref[:, cut] - mixed(
            res_c, jnp.concatenate([image, spread(second_ref, tile)], axis=1)
        )


def final_outputs(lines, coefs, right_sides, rhs, image, second):
    return pl.pallas_call(
        final_kernel,
        in_specs=[VMEM] * 6,
        out_specs=[VMEM] * 3,
        out_shape=[jax.ShapeDtypeStruct(right_sides.shape, F32)] * 2
        + [jax.ShapeDtypeStruct((1, HALF), F32)],
        name="final_outputs",
    )(lines, coefs, right_sides, rhs, image, second)


def exchanged(parts, axis):
    return lax.all_to_all(parts, axis, 0, 0, tiled=True)


def shared(value, axis):
    return exchanged(jnp.broadcast_to(value[None], (lax.axis_size(axis), *value.shape)), axis)


def on_device(points, noise_level, right_sides):
    rows, cols = lax.axis_size("row"), lax.axis_size(COL)
    col_index = lax.axis_index(COL)[None].astype(jnp.int32)
    row_units, col_units = own_units(points, rows, cols)
    row_pts = exchanged(row_units, "row")
    col_pts = exchanged(col_units, COL)
    rhs, noise = packed_rows(right_sides, noise_level)

    part = first_product(row_pts, col_pts, rhs)
    own = jnp.sum(exchanged(part, "row"), axis=0)
    raw = shared(own, COL).reshape(-1, LANES)
    part, image = second_product(col_index, row_pts, col_pts, raw, rhs, noise)
    own = jnp.sum(exchanged(part, "row"), axis=0)
    core = lax.axis_index(COL[-1])[None].astype(jnp.int32)
    share, second, coefs = middle(core, shared(own, COL), rhs, image, noise, rows)
    lines = lax.all_gather(jnp.sum(exchanged(share, "row"), axis=0), COL[-1])
    sol, res, norms = final_outputs(lines, coefs, right_sides, rhs, image, second)
    return sol, res, norms[0]


def solution(mesh):
    torus = Mesh(
        mesh.devices.reshape(mesh.shape["row"], 4, 4, 2), ("row", "col_0", "col_1", "col_2")
    )
    return jax.shard_map(
        on_device,
        mesh=torus,
        in_specs=(P(None, ROW_COL), P("row"), P(None, "row")),
        out_specs=(P(None, "row"), P(None, "row"), P()),
        check_vma=False,
    )
```

```python
import jax
import jax.numpy as jnp
from jax import lax
from jax.experimental import pallas as pl
from jax.experimental.pallas import tpu as pltpu
from jax.sharding import Mesh
from jax.sharding import PartitionSpec as P

COL = ("col_0", "col_1", "col_2")
ROW_COL = ("row", "col_0", "col_1", "col_2")
HIGH = lax.Precision.HIGHEST
F32 = jnp.float32
BF16 = jnp.bfloat16
THETA = 0.5
LANES = 128
HALF = 64
VMEM = pl.BlockSpec(memory_space=pltpu.VMEM)
SMEM = pl.BlockSpec(memory_space=pltpu.SMEM)
PARAMS = pltpu.CompilerParams(vmem_limit_bytes=16 * 1024 * 1024)


def lane_of(shape):
    return lax.broadcasted_iota(jnp.int32, shape, len(shape) - 1)


def packed(turned):
    return jnp.concatenate([turned[:32], turned[32:64]], axis=1)


def own_kernel(pts_ref, row_out, col_out):
    unit = jnp.concatenate([pts_ref[:4], pts_ref[4:]], axis=1)
    for place in range(row_out.shape[0]):
        row_out[place] = unit
    for place in range(col_out.shape[0]):
        col_out[place] = unit


def own_units(points, rows, cols):
    return pl.pallas_call(
        own_kernel,
        in_specs=[VMEM],
        out_specs=[VMEM] * 2,
        out_shape=[
            jax.ShapeDtypeStruct((rows, 4, LANES), F32),
            jax.ShapeDtypeStruct((cols, 4, LANES), F32),
        ],
        compiler_params=PARAMS,
        name="own_units",
    )(points)


def packed_kernel(rhs_ref, noise_ref, packed_out, noise_out):
    low = lane_of((32, LANES)) < HALF
    for tile in range(rhs_ref.shape[1] // LANES):
        turned = rhs_ref[:, tile * LANES : (tile + 1) * LANES].T
        noise = noise_ref[:, tile * LANES : (tile + 1) * LANES]
        noise = jnp.broadcast_to(noise, (LANES, LANES)).T
        for part in range(2):
            rows = slice(tile * 64 + part * 32, tile * 64 + part * 32 + 32)
            packed_out[rows] = packed(turned[part * 64 : part * 64 + 64])
            noise_out[rows] = jnp.where(
                low, noise[part * 64 : part * 64 + 32], noise[part * 64 + 32 : part * 64 + 64]
            )


def packed_rows(right_sides, noise_level):
    rows = right_sides.shape[1] // 2
    return pl.pallas_call(
        packed_kernel,
        in_specs=[VMEM] * 2,
        out_specs=[VMEM] * 2,
        out_shape=[jax.ShapeDtypeStruct((rows, LANES), F32)] * 2,
        cost_estimate=pl.CostEstimate(
            flops=4 * 10**9, bytes_accessed=3 * 4 * rows * LANES, transcendentals=0
        ),
        compiler_params=PARAMS,
        name="packed_rows",
    )(right_sides, noise_level[None, :])


def ordered(ref):
    place = lane_of((8, LANES)) // 32
    low = lane_of((4, LANES)) < HALF
    units = []
    for index in range(ref.shape[0]):
        unit = ref[index]
        turned = pltpu.roll(unit, HALF, 1)
        units.append(
            jnp.concatenate([jnp.where(low, unit, turned), jnp.where(low, turned, unit)], axis=0)
        )
    pieces = []
    for h in range(2):
        for start in range(0, len(units), 4):
            piece = None
            for q in range(4):
                unit = units[start + q]
                if (q - h) % 2:
                    unit = pltpu.roll(unit, 32, 1)
                piece = unit if piece is None else jnp.where(place == q, unit, piece)
            pieces.append(piece)
    return jnp.concatenate(pieces, axis=1)


def rounded(value):
    return value.astype(BF16).astype(F32)


def three_parts(value):
    first = rounded(value)
    rest = value - first
    second = rounded(rest)
    return first, second, rest - second


def augmented(pts, as_rows):
    x1, x2, x3 = three_parts(pts)
    half_sq = -0.5 * jnp.sum(pts * pts, axis=0, keepdims=True)
    s1, s2, s3 = three_parts(half_sq)
    sub = lax.broadcasted_iota(jnp.int32, pts.shape, 0)
    squares = jnp.where(sub == 0, s1, jnp.where(sub == 1, s2, jnp.where(sub == 2, s3, 0.0)))
    ones = jnp.where(sub < 3, 1.0, 0.0)
    zeros = jnp.zeros_like(pts)
    if as_rows:
        blocks = [x1, x1, x2, x2, x1, x3, x2, x3, squares, ones]
    else:
        blocks = [x1, x2, x1, x2, x3, x1, x3, x2, ones, squares]
    return jnp.concatenate(blocks + [zeros] * 6, axis=0)


def apply_kernel_matrix(out_pts, in_pts, values, result, left, right, stack):
    outs = left.shape[0]
    ins = right.shape[1]
    tile = min(512, outs // 2)
    for start in range(0, outs, LANES):
        piece = augmented(out_pts[:, start : start + LANES], True)
        left[start : start + LANES] = piece.T.astype(BF16)
    for start in range(0, ins, 256):
        right[:, start : start + 256] = augmented(in_pts[:, start : start + 256], False).astype(BF16)
    groups = ins // 256
    low = lane_of((LANES, LANES)) < HALF
    for group in range(groups):
        rows = values[group * LANES : (group + 1) * LANES]
        turned = pltpu.roll(rows, HALF, 1)
        for h in range(2):
            top = jnp.where(low, turned if h else rows, 0.0)
            bottom = jnp.where(low, 0.0, rows if h else turned)
            both = jnp.concatenate([top, bottom], axis=0)
            high = both.astype(BF16)
            rest = (both - high.astype(F32)).astype(BF16)
            stack[h * groups + group, :, :LANES] = high
            stack[h * groups + group, :, LANES:] = rest
    result[...] = jnp.zeros_like(result)
    pairs = ins // 256

    def step(index, carry):
        at = pl.multiple_of(lax.div(index, pairs) * tile, tile)
        pair = lax.rem(index, pairs)
        columns = right[:, pl.ds(pl.multiple_of(pair * 256, 256), 256)]
        highs, lows = [], []
        for h in range(2):
            lines = left[pl.ds(h * (outs // 2) + at, tile)]
            kernel = jnp.exp(jnp.dot(lines, columns, preferred_element_type=F32))
            high = kernel.astype(BF16)
            highs.append(high)
            lows.append((kernel - high.astype(F32)).astype(BF16))
        total = result[pl.ds(at, tile)]
        for a in range(2):
            weights = stack[pair * 2 + a]
            cut = slice(a * LANES, (a + 1) * LANES)
            high = jnp.concatenate([highs[0][:, cut], highs[1][:, cut]], axis=1)
            rest = jnp.concatenate([lows[0][:, cut], lows[1][:, cut]], axis=1)
            both = jnp.dot(high, weights, preferred_element_type=F32)
            total = total + both[:, :LANES] + both[:, LANES:]
            total = total + jnp.dot(rest, weights[:, :LANES], preferred_element_type=F32)
        result[pl.ds(at, tile)] = total
        return carry

    lax.fori_loop(0, (outs // 2 // tile) * pairs, step, 0)


def first_product_kernel(row_ref, col_ref, rhs_ref, out_ref, left, right, stack, result):
    apply_kernel_matrix(ordered(row_ref), ordered(col_ref), rhs_ref[...], result, left, right, stack)
    for place in range(out_ref.shape[0]):
        out_ref[place] = result[place * 32 : place * 32 + 32]


def second_product_kernel(
    place_ref, row_ref, col_ref, raw_ref, rhs_ref, noise_ref, out_ref, image_ref, left, right, stack, result, grams
):
    rhs = rhs_ref[...]
    image = raw_ref[...] + noise_ref[...] * rhs
    image_ref[...] = image
    values = rhs - THETA * image
    apply_kernel_matrix(ordered(row_ref), ordered(col_ref), values, result, left, right, stack)
    gram = gram_of(joined(two_parts(rhs), two_parts(image)))
    grams[0:32] = folded(summed_halves(gram[:LANES, :LANES]))
    grams[32:64] = folded(summed_halves(gram[:LANES, LANES:]))
    grams[64:96] = folded(summed_halves(gram[LANES:, LANES:]))
    lines = [grams[pl.ds(32 * m + place_ref[0], 1)] for m in range(3)]
    tail = jnp.concatenate(lines + [jnp.zeros((5, LANES), F32)], axis=0)
    for place in range(out_ref.shape[0]):
        out_ref[place, :32] = result[place * 32 : place * 32 + 32]
        out_ref[place, 32:] = tail


def product_scratch(outs, ins):
    return [
        pltpu.VMEM((outs, LANES), BF16),
        pltpu.VMEM((LANES, ins), BF16),
        pltpu.VMEM((ins // LANES, 256, 256), BF16),
        pltpu.VMEM((outs // 2, LANES), F32),
    ]


def product_cost(outs, ins):
    return pl.CostEstimate(
        flops=2 * outs * ins * 512, bytes_accessed=8 * (outs + ins) * HALF, transcendentals=outs * ins
    )


def first_product(row_pts, col_pts, rhs):
    outs, ins = row_pts.shape[0] * 64, col_pts.shape[0] * 64
    return pl.pallas_call(
        first_product_kernel,
        in_specs=[VMEM] * 3,
        out_specs=VMEM,
        out_shape=jax.ShapeDtypeStruct((row_pts.shape[0], 32, LANES), F32),
        scratch_shapes=product_scratch(outs, ins),
        cost_estimate=product_cost(outs, ins),
        compiler_params=PARAMS,
        name="first_product",
    )(row_pts, col_pts, rhs)


def second_product(place, row_pts, col_pts, raw, rhs, noise):
    outs, ins = row_pts.shape[0] * 64, col_pts.shape[0] * 64
    return pl.pallas_call(
        second_product_kernel,
        in_specs=[SMEM] + [VMEM] * 5,
        out_specs=[VMEM] * 2,
        out_shape=[
            jax.ShapeDtypeStruct((row_pts.shape[0], 40, LANES), F32),
            jax.ShapeDtypeStruct((ins // 2, LANES), F32),
        ],
        scratch_shapes=product_scratch(outs, ins) + [pltpu.VMEM((96, LANES), F32)],
        cost_estimate=product_cost(outs, ins),
        compiler_params=PARAMS,
        name="second_product",
    )(place, row_pts, col_pts, raw, rhs, noise)


def two_parts(value):
    high = value.astype(BF16)
    return high, (value - high.astype(F32)).astype(BF16)


def bf16_dot(first, second, first_dim, second_dim):
    dims = (((first_dim,), (second_dim,)), ((), ()))
    return lax.dot_general(first, second, dims, preferred_element_type=F32)


def parts_dot(first, second, first_dim=1, second_dim=0):
    high = bf16_dot(first[0], second[0], first_dim, second_dim)
    cross = bf16_dot(first[0], second[1], first_dim, second_dim)
    return high + cross + bf16_dot(first[1], second[0], first_dim, second_dim)


def gram_of(parts):
    high = bf16_dot(parts[0], parts[0], 0, 0)
    cross = bf16_dot(parts[0], parts[1], 0, 0)
    return high + cross + cross.T


def joined(*pairs):
    return tuple(jnp.concatenate([pair[i] for pair in pairs], axis=1) for i in range(2))


def summed_halves(gram):
    return gram[:HALF, :HALF] + gram[HALF:, HALF:]


def folded(square):
    return jnp.concatenate([square[:32], square[32:]], axis=1)


def unfolded(lines):
    return jnp.concatenate([lines[:, :HALF], lines[:, HALF:]], axis=0)


def row_and_column():
    shape = (HALF, HALF)
    return lax.broadcasted_iota(jnp.int32, shape, 0), lax.broadcasted_iota(jnp.int32, shape, 1)


def squares_of(first, second, third):
    row, column = row_and_column()
    diagonal = jnp.sum(jnp.where(row == column, second, 0.0), axis=0, keepdims=True)
    under = jnp.where(row == HALF - 1, diagonal, jnp.where(row == HALF - 2, diagonal[:, HALF - 1 :], 0.0))
    return jnp.where(column >= row, first, second), jnp.where(column >= row, third, under)


def matrices_of(upper, lower):
    row, column = row_and_column()
    turned, beneath = upper.T, lower.T
    diagonal = jnp.where(column == HALF - 1, lower[HALF - 2 : HALF - 1, :1], lower[HALF - 1 :])
    first = jnp.where(column >= row, upper, turned)
    second = jnp.where(column == row, diagonal, jnp.where(column < row, upper, turned))
    return first, second, jnp.where(column >= row, lower, beneath)


def small_dot(first, second):
    return jnp.dot(first, second, precision=HIGH, preferred_element_type=F32)


def twice(coefs):
    zero = jnp.zeros_like(coefs)
    return jnp.concatenate(
        [jnp.concatenate([coefs, zero], axis=1), jnp.concatenate([zero, coefs], axis=1)], axis=0
    )


def line(tile, index):
    return jnp.broadcast_to(tile[index : index + 1], tile.shape)


def solve_sym(*systems):
    sub = lax.broadcasted_iota(jnp.int32, (8, LANES), 0)
    state = []
    for matrix, target in systems:
        both = jnp.concatenate([0.5 * (matrix + matrix.T), target], axis=1)
        state.append(tuple(both[8 * t : 8 * t + 8] for t in range(8)))

    def step(group, state):
        state = [list(tiles) for tiles in state]
        for quad in range(2):
            lanes = [jnp.full((8, LANES), group * 8 + quad * 4 + j, jnp.int32) for j in range(4)]
            spread = [
                [[jnp.take_along_axis(tile, lane, axis=1) for tile in tiles] for lane in lanes] for tiles in state
            ]
            for j in range(4):
                at = quad * 4 + j
                here = sub == at
                for tiles, columns in zip(state, spread):
                    inverse = 1.0 / line(columns[j][0], at)
                    row = line(tiles[0], at) * inverse
                    for t in range(8):
                        new = tiles[t] - columns[j][t] * row
                        tiles[t] = jnp.where(here, row, new) if t == 0 else new
                    for later in range(j + 1, 4):
                        ratio = line(columns[later][0], at) * inverse
                        for t in range(8):
                            new = columns[later][t] - columns[j][t] * ratio
                            columns[later][t] = jnp.where(here, ratio, new) if t == 0 else new
        return tuple(tuple(tiles[1:] + tiles[:1]) for tiles in state)

    state = lax.fori_loop(0, 8, step, tuple(state))
    return [jnp.concatenate(tiles, axis=0)[:, HALF:] for tiles in state]


def middle_kernel(core_ref, unit_ref, rhs_ref, image_ref, noise_ref, share_ref, second_ref, coef_ref, lines):
    for place in range(unit_ref.shape[0]):
        tail = unit_ref[place, 32:]
        for m in range(3):
            lines[32 * m + place : 32 * m + place + 1] = tail[m : m + 1]
    gram, curv, square = (unfolded(lines[32 * m : 32 * m + 32]) for m in range(3))
    row, column = row_and_column()
    eye = jnp.where(row == column, 1.0, 0.0)
    coef0, inverse = solve_sym((curv, gram), (gram, eye))
    cross = small_dot(curv, coef0)
    gram1 = gram - cross - cross.T + small_dot(coef0.T, small_dot(square, coef0))
    dcoef = small_dot(inverse, gram1)
    rhs, image = rhs_ref[...], image_ref[...]
    raw = jnp.concatenate([unit_ref[i, :32] for i in range(unit_ref.shape[0])], axis=0)
    second = raw + noise_ref[...] * (rhs - THETA * image)
    second_ref[...] = second
    scaled = coef0 * (1.0 / THETA)
    down = -twice(coef0)
    turn = twice(dcoef)
    mix = jnp.concatenate(
        [
            jnp.concatenate([turn, jnp.zeros_like(turn)], axis=1),
            jnp.concatenate([down, down], axis=1),
        ],
        axis=0,
    )
    mix1 = jnp.concatenate([twice(eye - scaled + dcoef), twice(scaled)], axis=0)
    rhs_parts, image_parts = two_parts(rhs), two_parts(image)
    change = parts_dot(joined(rhs_parts, image_parts), two_parts(mix))
    direction, residual = rhs + change[:, :LANES], rhs + change[:, LANES:]
    image1 = two_parts(parts_dot(joined(image_parts, two_parts(second)), two_parts(mix1)))
    crossed = parts_dot(joined(two_parts(direction), image1), image1, 0, 0)
    curv1 = summed_halves(crossed[:LANES])
    upper, lower = squares_of(
        0.5 * (curv1 + curv1.T),
        summed_halves(gram_of(two_parts(residual))),
        summed_halves(crossed[LANES:]),
    )
    lines[0:32] = folded(upper)
    lines[32:64] = folded(lower)
    start = pl.multiple_of(core_ref[0] * 16, 16)
    part = jnp.concatenate([lines[pl.ds(32 * m + start, 16)] for m in range(2)], axis=0)
    for place in range(share_ref.shape[0]):
        share_ref[place] = part
    coef_ref[0:64] = jnp.concatenate([coef0, dcoef], axis=1)
    coef_ref[64:128] = jnp.concatenate([gram, eye], axis=1)


def middle(core, units, rhs, image, noise, rows):
    return pl.pallas_call(
        middle_kernel,
        in_specs=[SMEM] + [VMEM] * 4,
        out_specs=[VMEM] * 3,
        out_shape=[
            jax.ShapeDtypeStruct((rows, 32, LANES), F32),
            jax.ShapeDtypeStruct(rhs.shape, F32),
            jax.ShapeDtypeStruct((128, LANES), F32),
        ],
        scratch_shapes=[pltpu.VMEM((96, LANES), F32)],
        compiler_params=PARAMS,
        name="middle",
    )(core, units, rhs, image, noise)


def final_kernel(lines_ref, coef_ref, rhs_ref, packed_ref, image_ref, second_ref, sol_ref, res_ref, norm_ref):
    low = lane_of((32, LANES)) < HALF
    upper, lower = (
        unfolded(jnp.concatenate([lines_ref[half, 16 * m : 16 * m + 16] for half in range(2)], axis=0))
        for m in range(2)
    )
    curv1, gram1, square = matrices_of(upper, lower)
    coef0, dcoef = coef_ref[0:64, :HALF], coef_ref[0:64, HALF:]
    gram, eye = coef_ref[64:128, :HALF], coef_ref[64:128, HALF:]
    (coef1,) = solve_sym((curv1, gram1))
    cross = small_dot(curv1, coef1)
    gram2 = gram1 - cross - cross.T + small_dot(coef1.T, small_dot(square, coef1))
    norms = jnp.sum(eye * gram2, axis=0, keepdims=True) / jnp.sum(eye * gram, axis=0, keepdims=True)
    norm_ref[...] = jnp.sqrt(jnp.maximum(norms, 0.0))
    linear = coef0 + coef1 + small_dot(dcoef, coef1)
    quadratic = small_dot(coef0, coef1)
    scaled = quadratic * (1.0 / THETA)

    def doubled(first, second):
        first, second = first.T, second.T
        high, rest = two_parts(jnp.concatenate([first, first, second, second], axis=1))
        return jnp.concatenate([high, rest], axis=0)

    sol_c = doubled(linear, -quadratic)
    res_c = doubled(linear - scaled, scaled)

    def spread(ref, start):
        pieces = []
        for part in range(4):
            rows = ref[start // 2 + part * 32 : start // 2 + part * 32 + 32]
            pieces += [jnp.where(low, rows, 0.0), jnp.where(low, 0.0, rows)]
        return two_parts(jnp.concatenate(pieces, axis=0))

    def mixed(coefs, pair):
        both = bf16_dot(coefs, pair[0], 1, 1)
        return both[:HALF] + both[HALF:] + bf16_dot(coefs[:HALF], pair[1], 1, 1)

    for start in range(0, rhs_ref.shape[1], 256):
        cut = slice(start, start + 256)
        image = spread(image_ref, start)
        sol_ref[:, cut] = mixed(sol_c, joined(spread(packed_ref, start), image))
        res_ref[:, cut] = rhs_ref[:, cut] - mixed(res_c, joined(image, spread(second_ref, start)))


def final_outputs(lines, coefs, right_sides, rhs, image, second):
    return pl.pallas_call(
        final_kernel,
        in_specs=[VMEM] * 6,
        out_specs=[VMEM] * 3,
        out_shape=[jax.ShapeDtypeStruct(right_sides.shape, F32)] * 2
        + [jax.ShapeDtypeStruct((1, HALF), F32)],
        compiler_params=PARAMS,
        name="final_outputs",
    )(lines, coefs, right_sides, rhs, image, second)


def exchanged(parts, axis):
    return lax.all_to_all(parts, axis, 0, 0, tiled=True)


def shared(value, axis):
    return exchanged(jnp.broadcast_to(value[None], (lax.axis_size(axis), *value.shape)), axis)


def on_device(points, noise_level, right_sides):
    rows, cols = lax.axis_size("row"), lax.axis_size(COL)
    col_index = lax.axis_index(COL)[None].astype(jnp.int32)
    row_units, col_units = own_units(points, rows, cols)
    row_pts = exchanged(row_units, "row")
    col_pts = exchanged(col_units, COL)
    rhs, noise = packed_rows(right_sides, noise_level)

    part = first_product(row_pts, col_pts, rhs)
    own = jnp.sum(exchanged(part, "row"), axis=0)
    raw = shared(own, COL).reshape(-1, LANES)
    part, image = second_product(col_index, row_pts, col_pts, raw, rhs, noise)
    own = jnp.sum(exchanged(part, "row"), axis=0)
    core = lax.axis_index(COL[-1])[None].astype(jnp.int32)
    share, second, coefs = middle(core, shared(own, COL), rhs, image, noise, rows)
    lines = lax.all_gather(jnp.sum(exchanged(share, "row"), axis=0), COL[-1])
    sol, res, norms = final_outputs(lines, coefs, right_sides, rhs, image, second)
    return sol, res, norms[0]


def solution(mesh):
    torus = Mesh(
        mesh.devices.reshape(mesh.shape["row"], 4, 4, 2), ("row", "col_0", "col_1", "col_2")
    )
    return jax.shard_map(
        on_device,
        mesh=torus,
        in_specs=(P(None, ROW_COL), P("row"), P(None, "row")),
        out_specs=(P(None, "row"), P(None, "row"), P()),
        check_vma=False,
    )
```

```python
import jax
import jax.numpy as jnp
from jax import lax
from jax.experimental import pallas as pl
from jax.experimental.pallas import tpu as pltpu
from jax.sharding import Mesh
from jax.sharding import PartitionSpec as P

COL = ("col_0", "col_1", "col_2")
ROW_COL = ("row", "col_0", "col_1", "col_2")
HIGH = lax.Precision.HIGHEST
F32 = jnp.float32
BF16 = jnp.bfloat16
THETA = 0.5
LANES = 128
HALF = 64
VMEM = pl.BlockSpec(memory_space=pltpu.VMEM)
PARAMS = pltpu.CompilerParams(vmem_limit_bytes=16 * 1024 * 1024)


def lane_of(shape):
    return lax.broadcasted_iota(jnp.int32, shape, len(shape) - 1)


def packed(turned):
    return jnp.concatenate([turned[:32], turned[32:64]], axis=1)


def prepare_kernel(
    pts_hbm, rhs_hbm, noise_hbm, row_out, col_out, packed_out, noise_out, pts_ref, rhs_ref, noise_ref, sems
):
    copies = [
        pltpu.make_async_copy(source, target, sems.at[i])
        for i, (source, target) in enumerate(((pts_hbm, pts_ref), (noise_hbm, noise_ref), (rhs_hbm, rhs_ref)))
    ]
    for copy in copies:
        copy.start()
    copies[0].wait()
    unit = jnp.concatenate([pts_ref[:4], pts_ref[4:]], axis=1)
    for place in range(row_out.shape[0]):
        row_out[place] = unit
    for place in range(col_out.shape[0]):
        col_out[place] = unit
    copies[1].wait()
    low = lane_of((32, LANES)) < HALF
    for tile in range(rhs_ref.shape[1] // LANES):
        noise = noise_ref[:, tile * LANES : (tile + 1) * LANES]
        noise = jnp.broadcast_to(noise, (LANES, LANES)).T
        for part in range(2):
            rows = slice(tile * 64 + part * 32, tile * 64 + part * 32 + 32)
            noise_out[rows] = jnp.where(
                low, noise[part * 64 : part * 64 + 32], noise[part * 64 + 32 : part * 64 + 64]
            )
    copies[2].wait()
    for tile in range(rhs_ref.shape[1] // LANES):
        turned = rhs_ref[:, tile * LANES : (tile + 1) * LANES].T
        for part in range(2):
            rows = slice(tile * 64 + part * 32, tile * 64 + part * 32 + 32)
            packed_out[rows] = packed(turned[part * 64 : part * 64 + 64])


def prepare(points, right_sides, noise_level, rows, cols):
    lines = right_sides.shape[1] // 2
    noise_row = noise_level[None, :]
    return pl.pallas_call(
        prepare_kernel,
        in_specs=[pl.BlockSpec(memory_space=pltpu.HBM)] * 3,
        out_specs=[VMEM] * 4,
        out_shape=[
            jax.ShapeDtypeStruct((rows, 4, LANES), F32),
            jax.ShapeDtypeStruct((cols, 4, LANES), F32),
            jax.ShapeDtypeStruct((lines, LANES), F32),
            jax.ShapeDtypeStruct((lines, LANES), F32),
        ],
        scratch_shapes=[
            pltpu.VMEM(points.shape, F32),
            pltpu.VMEM(right_sides.shape, F32),
            pltpu.VMEM(noise_row.shape, F32),
            pltpu.SemaphoreType.DMA((3,)),
        ],
        compiler_params=PARAMS,
        name="prepare",
    )(points, right_sides, noise_row)


def ordered(ref):
    place = lane_of((8, LANES)) // 32
    low = lane_of((4, LANES)) < HALF
    units = []
    for index in range(ref.shape[0]):
        unit = ref[index]
        turned = pltpu.roll(unit, HALF, 1)
        units.append(
            jnp.concatenate([jnp.where(low, unit, turned), jnp.where(low, turned, unit)], axis=0)
        )
    pieces = []
    for h in range(2):
        for start in range(0, len(units), 4):
            piece = None
            for q in range(4):
                unit = units[start + q]
                if (q - h) % 2:
                    unit = pltpu.roll(unit, 32, 1)
                piece = unit if piece is None else jnp.where(place == q, unit, piece)
            pieces.append(piece)
    return jnp.concatenate(pieces, axis=1)


def rounded(value):
    return value.astype(BF16).astype(F32)


def three_parts(value):
    first = rounded(value)
    rest = value - first
    second = rounded(rest)
    return first, second, rest - second


def augmented(pts, as_rows):
    x1, x2, x3 = three_parts(pts)
    half_sq = -0.5 * jnp.sum(pts * pts, axis=0, keepdims=True)
    s1, s2, s3 = three_parts(half_sq)
    sub = lax.broadcasted_iota(jnp.int32, pts.shape, 0)
    squares = jnp.where(sub == 0, s1, jnp.where(sub == 1, s2, jnp.where(sub == 2, s3, 0.0)))
    ones = jnp.where(sub < 3, 1.0, 0.0)
    zeros = jnp.zeros_like(pts)
    if as_rows:
        blocks = [x1, x1, x2, x2, x1, x3, x2, x3, squares, ones]
    else:
        blocks = [x1, x2, x1, x2, x3, x1, x3, x2, ones, squares]
    return jnp.concatenate(blocks + [zeros] * 6, axis=0)


def stack_values(values, stack):
    groups = values.shape[0] // LANES
    low = lane_of((LANES, LANES)) < HALF
    for group in range(groups):
        rows = values[group * LANES : (group + 1) * LANES]
        turned = pltpu.roll(rows, HALF, 1)
        for h in range(2):
            top = jnp.where(low, turned if h else rows, 0.0)
            bottom = jnp.where(low, 0.0, rows if h else turned)
            high, rest = two_parts(jnp.concatenate([top, bottom], axis=0))
            stack[h * groups + group, :, :LANES] = high
            stack[h * groups + group, :, LANES:] = rest


def apply_kernel_matrix(out_pts, in_pts, values, result, left, right, stack):
    outs, ins = left.shape[0], right.shape[1]
    for start in range(0, outs, LANES):
        piece = augmented(out_pts[:, start : start + LANES], True)
        left[start : start + LANES] = piece.T.astype(BF16)
    for start in range(0, ins, 256):
        right[:, start : start + 256] = augmented(in_pts[:, start : start + 256], False).astype(BF16)
    stack_values(values, stack)
    result[...] = jnp.zeros_like(result)
    tile = min(512, outs // 2)
    pairs = ins // 256

    def step(index, carry):
        at = pl.multiple_of(lax.div(index, pairs) * tile, tile)
        pair = lax.rem(index, pairs)
        columns = right[:, pl.ds(pl.multiple_of(pair * 256, 256), 256)]
        halves = []
        for h in range(2):
            lines = left[pl.ds(h * (outs // 2) + at, tile)]
            halves.append(two_parts(jnp.exp(bf16_dot(lines, columns, 1, 0))))
        total = result[pl.ds(at, tile)]
        for a in range(2):
            cut = slice(a * LANES, (a + 1) * LANES)
            high, low = (
                jnp.concatenate([halves[0][part][:, cut], halves[1][part][:, cut]], axis=1) for part in range(2)
            )
            weights = stack[pair * 2 + a]
            both = bf16_dot(high, weights, 1, 0)
            total = total + both[:, :LANES] + both[:, LANES:]
            total = total + bf16_dot(low, weights[:, :LANES], 1, 0)
        result[pl.ds(at, tile)] = total
        return carry

    lax.fori_loop(0, (outs // 2 // tile) * pairs, step, 0)


def first_product_kernel(row_ref, col_ref, rhs_ref, out_ref, left, right, stack, result):
    apply_kernel_matrix(ordered(row_ref), ordered(col_ref), rhs_ref[...], result, left, right, stack)
    for place in range(out_ref.shape[0]):
        out_ref[place] = result[place * 32 : place * 32 + 32]


def second_product_kernel(
    row_ref, col_ref, raw_ref, rhs_ref, noise_ref, out_ref, image_ref, left, right, stack, result, grams
):
    rhs = rhs_ref[...]
    image = raw_ref[...] + noise_ref[...] * rhs
    image_ref[...] = image
    values = rhs - THETA * image
    apply_kernel_matrix(ordered(row_ref), ordered(col_ref), values, result, left, right, stack)
    gram = gram_of(joined(two_parts(rhs), two_parts(image)))
    grams[0:32] = folded(summed_halves(gram[:LANES, :LANES]))
    grams[32:64] = folded(summed_halves(gram[:LANES, LANES:]))
    grams[64:96] = folded(summed_halves(gram[LANES:, LANES:]))
    own = lax.axis_index(COL)
    lines = [grams[pl.ds(32 * m + own, 1)] for m in range(3)]
    tail = jnp.concatenate(lines + [jnp.zeros((1, LANES), F32)], axis=0)
    for place in range(out_ref.shape[0]):
        for quad in range(8):
            start = place * 32 + quad * 4
            out_ref[place, quad] = result[start : start + 4]
        out_ref[place, 8] = tail


def product_scratch(outs, ins):
    return [
        pltpu.VMEM((outs, LANES), BF16),
        pltpu.VMEM((LANES, ins), BF16),
        pltpu.VMEM((ins // LANES, 256, 256), BF16),
        pltpu.VMEM((outs // 2, LANES), F32),
    ]


def product_cost(outs, ins):
    return pl.CostEstimate(
        flops=2 * outs * ins * 512, bytes_accessed=8 * (outs + ins) * HALF, transcendentals=outs * ins
    )


def first_product(row_pts, col_pts, rhs):
    outs, ins = row_pts.shape[0] * 64, col_pts.shape[0] * 64
    return pl.pallas_call(
        first_product_kernel,
        in_specs=[VMEM] * 3,
        out_specs=VMEM,
        out_shape=jax.ShapeDtypeStruct((row_pts.shape[0], 32, LANES), F32),
        scratch_shapes=product_scratch(outs, ins),
        cost_estimate=product_cost(outs, ins),
        compiler_params=PARAMS,
        name="first_product",
    )(row_pts, col_pts, rhs)


def second_product(row_pts, col_pts, raw, rhs, noise):
    outs, ins = row_pts.shape[0] * 64, col_pts.shape[0] * 64
    return pl.pallas_call(
        second_product_kernel,
        in_specs=[VMEM] * 5,
        out_specs=[VMEM] * 2,
        out_shape=[
            jax.ShapeDtypeStruct((row_pts.shape[0], 9, 4, LANES), F32),
            jax.ShapeDtypeStruct((ins // 2, LANES), F32),
        ],
        scratch_shapes=product_scratch(outs, ins) + [pltpu.VMEM((96, LANES), F32)],
        cost_estimate=product_cost(outs, ins),
        compiler_params=PARAMS,
        name="second_product",
    )(row_pts, col_pts, raw, rhs, noise)


def two_parts(value):
    high = value.astype(BF16)
    return high, (value - high.astype(F32)).astype(BF16)


def bf16_dot(first, second, first_dim, second_dim):
    dims = (((first_dim,), (second_dim,)), ((), ()))
    return lax.dot_general(first, second, dims, preferred_element_type=F32)


def parts_dot(first, second, first_dim=1, second_dim=0):
    high = bf16_dot(first[0], second[0], first_dim, second_dim)
    cross = bf16_dot(first[0], second[1], first_dim, second_dim)
    return high + cross + bf16_dot(first[1], second[0], first_dim, second_dim)


def gram_of(parts):
    high = bf16_dot(parts[0], parts[0], 0, 0)
    cross = bf16_dot(parts[0], parts[1], 0, 0)
    return high + cross + cross.T


def joined(*pairs):
    return tuple(jnp.concatenate([pair[i] for pair in pairs], axis=1) for i in range(2))


def summed_halves(gram):
    return gram[:HALF, :HALF] + gram[HALF:, HALF:]


def folded(square):
    return jnp.concatenate([square[:32], square[32:]], axis=1)


def unfolded(lines):
    return jnp.concatenate([lines[:, :HALF], lines[:, HALF:]], axis=0)


def row_and_column():
    shape = (HALF, HALF)
    return lax.broadcasted_iota(jnp.int32, shape, 0), lax.broadcasted_iota(jnp.int32, shape, 1)


def squares_of(first, second, third):
    row, column = row_and_column()
    diagonal = jnp.sum(jnp.where(row == column, second, 0.0), axis=0, keepdims=True)
    under = jnp.where(row == HALF - 1, diagonal, jnp.where(row == HALF - 2, diagonal[:, HALF - 1 :], 0.0))
    return jnp.where(column >= row, first, second), jnp.where(column >= row, third, under)


def matrices_of(upper, lower):
    row, column = row_and_column()
    turned, beneath = upper.T, lower.T
    diagonal = jnp.where(column == HALF - 1, lower[HALF - 2 : HALF - 1, :1], lower[HALF - 1 :])
    first = jnp.where(column >= row, upper, turned)
    second = jnp.where(column == row, diagonal, jnp.where(column < row, upper, turned))
    return first, second, jnp.where(column >= row, lower, beneath)


def small_dot(first, second):
    return jnp.dot(first, second, precision=HIGH, preferred_element_type=F32)


def twice(coefs):
    zero = jnp.zeros_like(coefs)
    return jnp.concatenate(
        [jnp.concatenate([coefs, zero], axis=1), jnp.concatenate([zero, coefs], axis=1)], axis=0
    )


def line(tile, index):
    return jnp.broadcast_to(tile[index : index + 1], tile.shape)


def solve_sym(*systems):
    sub = lax.broadcasted_iota(jnp.int32, (8, LANES), 0)
    state = []
    for matrix, target in systems:
        both = jnp.concatenate([0.5 * (matrix + matrix.T), target], axis=1)
        state.append(tuple(both[8 * t : 8 * t + 8] for t in range(8)))

    def step(group, state):
        state = [list(tiles) for tiles in state]
        for quad in range(2):
            lanes = [jnp.full((8, LANES), group * 8 + quad * 4 + j, jnp.int32) for j in range(4)]
            spread = [
                [[jnp.take_along_axis(tile, lane, axis=1) for tile in tiles] for lane in lanes] for tiles in state
            ]
            for j in range(4):
                at = quad * 4 + j
                here = sub == at
                for tiles, columns in zip(state, spread):
                    inverse = 1.0 / line(columns[j][0], at)
                    row = line(tiles[0], at) * inverse
                    for t in range(8):
                        new = tiles[t] - columns[j][t] * row
                        tiles[t] = jnp.where(here, row, new) if t == 0 else new
                    for later in range(j + 1, 4):
                        ratio = line(columns[later][0], at) * inverse
                        for t in range(8):
                            new = columns[later][t] - columns[j][t] * ratio
                            columns[later][t] = jnp.where(here, ratio, new) if t == 0 else new
        return tuple(tuple(tiles[1:] + tiles[:1]) for tiles in state)

    state = lax.fori_loop(0, 8, step, tuple(state))
    return [jnp.concatenate(tiles, axis=0)[:, HALF:] for tiles in state]


def middle_kernel(unit_ref, rhs_ref, image_ref, noise_ref, share_ref, second_ref, coef_ref, lines):
    for place in range(unit_ref.shape[0]):
        tail = unit_ref[place, 8]
        for m in range(3):
            lines[32 * m + place : 32 * m + place + 1] = tail[m : m + 1]
    gram, curv, square = (unfolded(lines[32 * m : 32 * m + 32]) for m in range(3))
    row, column = row_and_column()
    eye = jnp.where(row == column, 1.0, 0.0)
    coef0, inverse = solve_sym((curv, gram), (gram, eye))
    cross = small_dot(curv, coef0)
    gram1 = gram - cross - cross.T + small_dot(coef0.T, small_dot(square, coef0))
    dcoef = small_dot(inverse, gram1)
    rhs, image = rhs_ref[...], image_ref[...]
    raw = jnp.concatenate([unit_ref[i, quad] for i in range(unit_ref.shape[0]) for quad in range(8)], axis=0)
    second = raw + noise_ref[...] * (rhs - THETA * image)
    second_ref[...] = second
    scaled = coef0 * (1.0 / THETA)
    down = -twice(coef0)
    turn = twice(dcoef)
    mix = jnp.concatenate(
        [
            jnp.concatenate([turn, jnp.zeros_like(turn)], axis=1),
            jnp.concatenate([down, down], axis=1),
        ],
        axis=0,
    )
    mix1 = jnp.concatenate([twice(eye - scaled + dcoef), twice(scaled)], axis=0)
    rhs_parts, image_parts = two_parts(rhs), two_parts(image)
    change = parts_dot(joined(rhs_parts, image_parts), two_parts(mix))
    direction, residual = rhs + change[:, :LANES], rhs + change[:, LANES:]
    image1 = two_parts(parts_dot(joined(image_parts, two_parts(second)), two_parts(mix1)))
    crossed = parts_dot(joined(two_parts(direction), image1), image1, 0, 0)
    curv1 = summed_halves(crossed[:LANES])
    upper, lower = squares_of(
        0.5 * (curv1 + curv1.T),
        summed_halves(gram_of(two_parts(residual))),
        summed_halves(crossed[LANES:]),
    )
    lines[0:32] = folded(upper)
    lines[32:64] = folded(lower)
    start = pl.multiple_of(lax.axis_index(COL[-1]) * 16, 16)
    part = jnp.concatenate([lines[pl.ds(32 * m + start, 16)] for m in range(2)], axis=0)
    for place in range(share_ref.shape[0]):
        share_ref[place] = part
    coef_ref[0:64] = jnp.concatenate([coef0, dcoef], axis=1)
    coef_ref[64:128] = jnp.concatenate([gram, eye], axis=1)


def middle(units, rhs, image, noise, rows):
    return pl.pallas_call(
        middle_kernel,
        in_specs=[VMEM] * 4,
        out_specs=[VMEM] * 3,
        out_shape=[
            jax.ShapeDtypeStruct((rows, 32, LANES), F32),
            jax.ShapeDtypeStruct(rhs.shape, F32),
            jax.ShapeDtypeStruct((128, LANES), F32),
        ],
        scratch_shapes=[pltpu.VMEM((96, LANES), F32)],
        compiler_params=PARAMS,
        name="middle",
    )(units, rhs, image, noise)


def final_kernel(lines_ref, coef_ref, rhs_ref, packed_ref, image_ref, second_ref, sol_ref, res_ref, norm_ref):
    low = lane_of((32, LANES)) < HALF
    upper, lower = (
        unfolded(jnp.concatenate([lines_ref[half, 16 * m : 16 * m + 16] for half in range(2)], axis=0))
        for m in range(2)
    )
    curv1, gram1, square = matrices_of(upper, lower)
    coef0, dcoef = coef_ref[0:64, :HALF], coef_ref[0:64, HALF:]
    gram, eye = coef_ref[64:128, :HALF], coef_ref[64:128, HALF:]
    (coef1,) = solve_sym((curv1, gram1))
    cross = small_dot(curv1, coef1)
    gram2 = gram1 - cross - cross.T + small_dot(coef1.T, small_dot(square, coef1))
    norms = jnp.sum(eye * gram2, axis=0, keepdims=True) / jnp.sum(eye * gram, axis=0, keepdims=True)
    norm_ref[...] = jnp.sqrt(jnp.maximum(norms, 0.0))
    linear = coef0 + coef1 + small_dot(dcoef, coef1)
    quadratic = small_dot(coef0, coef1)
    scaled = quadratic * (1.0 / THETA)

    def doubled(first, second):
        first, second = first.T, second.T
        high, rest = two_parts(jnp.concatenate([first, first, second, second], axis=1))
        return jnp.concatenate([high, rest], axis=0)

    sol_c = doubled(linear, -quadratic)
    res_c = doubled(linear - scaled, scaled)

    def spread(ref, start):
        pieces = []
        for part in range(4):
            rows = ref[start // 2 + part * 32 : start // 2 + part * 32 + 32]
            pieces += [jnp.where(low, rows, 0.0), jnp.where(low, 0.0, rows)]
        return two_parts(jnp.concatenate(pieces, axis=0))

    def mixed(coefs, pair):
        both = bf16_dot(coefs, pair[0], 1, 1)
        return both[:HALF] + both[HALF:] + bf16_dot(coefs[:HALF], pair[1], 1, 1)

    for start in range(0, rhs_ref.shape[1], 256):
        cut = slice(start, start + 256)
        image = spread(image_ref, start)
        sol_ref[:, cut] = mixed(sol_c, joined(spread(packed_ref, start), image))
        res_ref[:, cut] = rhs_ref[:, cut] - mixed(res_c, joined(image, spread(second_ref, start)))


def final_outputs(lines, coefs, right_sides, rhs, image, second):
    return pl.pallas_call(
        final_kernel,
        in_specs=[VMEM] * 6,
        out_specs=[VMEM] * 3,
        out_shape=[jax.ShapeDtypeStruct(right_sides.shape, F32)] * 2
        + [jax.ShapeDtypeStruct((1, HALF), F32)],
        compiler_params=PARAMS,
        name="final_outputs",
    )(lines, coefs, right_sides, rhs, image, second)


def exchanged(parts, axis):
    return lax.all_to_all(parts, axis, 0, 0, tiled=True)


def shared(value, axis):
    return exchanged(jnp.broadcast_to(value[None], (lax.axis_size(axis), *value.shape)), axis)


def on_device(points, noise_level, right_sides):
    rows, cols = lax.axis_size("row"), lax.axis_size(COL)
    row_units, col_units, rhs, noise = prepare(points, right_sides, noise_level, rows, cols)
    col_pts = exchanged(col_units, COL)
    row_pts = exchanged(row_units, "row")

    part = first_product(row_pts, col_pts, rhs)
    own = jnp.sum(exchanged(part, "row"), axis=0)
    raw = shared(own, COL).reshape(-1, LANES)
    part, image = second_product(row_pts, col_pts, raw, rhs, noise)
    own = jnp.sum(exchanged(part, "row"), axis=0)
    share, second, coefs = middle(shared(own, COL), rhs, image, noise, rows)
    lines = lax.all_gather(jnp.sum(exchanged(share, "row"), axis=0), COL[-1])
    sol, res, norms = final_outputs(lines, coefs, right_sides, rhs, image, second)
    return sol, res, norms[0]


def solution(mesh):
    torus = Mesh(
        mesh.devices.reshape(mesh.shape["row"], 4, 4, 2), ("row", "col_0", "col_1", "col_2")
    )
    return jax.shard_map(
        on_device,
        mesh=torus,
        in_specs=(P(None, ROW_COL), P("row"), P(None, "row")),
        out_specs=(P(None, "row"), P(None, "row"), P()),
        check_vma=False,
    )
```

```python
import jax
import jax.numpy as jnp
from jax import lax
from jax.experimental import pallas as pl
from jax.experimental.pallas import tpu as pltpu
from jax.sharding import Mesh
from jax.sharding import PartitionSpec as P

COL = ("col_0", "col_1", "col_2")
ROW_COL = ("row", "col_0", "col_1", "col_2")
HIGH = lax.Precision.HIGHEST
F32 = jnp.float32
BF16 = jnp.bfloat16
THETA = 0.5
LANES = 128
HALF = 64
VMEM = pl.BlockSpec(memory_space=pltpu.VMEM)
PARAMS = pltpu.CompilerParams(vmem_limit_bytes=16 * 1024 * 1024)


def lane_of(shape):
    return lax.broadcasted_iota(jnp.int32, shape, len(shape) - 1)


def packed(turned):
    return jnp.concatenate([turned[:32], turned[32:64]], axis=1)


def own_kernel(pts_ref, row_out, col_out):
    unit = jnp.concatenate([pts_ref[:4], pts_ref[4:]], axis=1)
    for place in range(row_out.shape[0]):
        row_out[place] = unit
    for place in range(col_out.shape[0]):
        col_out[place] = unit


def own_units(points, rows, cols):
    return pl.pallas_call(
        own_kernel,
        in_specs=[VMEM],
        out_specs=[VMEM] * 2,
        out_shape=[
            jax.ShapeDtypeStruct((rows, 4, LANES), F32),
            jax.ShapeDtypeStruct((cols, 4, LANES), F32),
        ],
        compiler_params=PARAMS,
        name="own_units",
    )(points)


def prepare_kernel(rhs_ref, noise_ref, packed_out, noise_out):
    low = lane_of((32, LANES)) < HALF
    for tile in range(rhs_ref.shape[1] // LANES):
        turned = rhs_ref[:, tile * LANES : (tile + 1) * LANES].T
        noise = noise_ref[:, tile * LANES : (tile + 1) * LANES]
        noise = jnp.broadcast_to(noise, (LANES, LANES)).T
        for part in range(2):
            rows = slice(tile * 64 + part * 32, tile * 64 + part * 32 + 32)
            packed_out[rows] = packed(turned[part * 64 : part * 64 + 64])
            noise_out[rows] = jnp.where(
                low, noise[part * 64 : part * 64 + 32], noise[part * 64 + 32 : part * 64 + 64]
            )


def prepare(right_sides, noise_level):
    ins = right_sides.shape[1]
    return pl.pallas_call(
        prepare_kernel,
        in_specs=[VMEM] * 2,
        out_specs=[VMEM] * 2,
        out_shape=[jax.ShapeDtypeStruct((ins // 2, LANES), F32)] * 2,
        cost_estimate=pl.CostEstimate(flops=4 * 10**9, bytes_accessed=6 * 10**6, transcendentals=0),
        compiler_params=PARAMS,
        name="prepare",
    )(right_sides, noise_level[None, :])


def ordered(ref):
    place = lane_of((8, LANES)) // 32
    low = lane_of((4, LANES)) < HALF
    units = []
    for index in range(ref.shape[0]):
        unit = ref[index]
        turned = pltpu.roll(unit, HALF, 1)
        units.append(
            jnp.concatenate([jnp.where(low, unit, turned), jnp.where(low, turned, unit)], axis=0)
        )
    pieces = []
    for h in range(2):
        for start in range(0, len(units), 4):
            piece = None
            for q in range(4):
                unit = units[start + q]
                if (q - h) % 2:
                    unit = pltpu.roll(unit, 32, 1)
                piece = unit if piece is None else jnp.where(place == q, unit, piece)
            pieces.append(piece)
    return jnp.concatenate(pieces, axis=1)


def rounded(value):
    return value.astype(BF16).astype(F32)


def three_parts(value):
    first = rounded(value)
    rest = value - first
    second = rounded(rest)
    return first, second, rest - second


def augmented(pts, as_rows):
    x1, x2, x3 = three_parts(pts)
    half_sq = -0.5 * jnp.sum(pts * pts, axis=0, keepdims=True)
    s1, s2, s3 = three_parts(half_sq)
    sub = lax.broadcasted_iota(jnp.int32, pts.shape, 0)
    squares = jnp.where(sub == 0, s1, jnp.where(sub == 1, s2, jnp.where(sub == 2, s3, 0.0)))
    ones = jnp.where(sub < 3, 1.0, 0.0)
    zeros = jnp.zeros_like(pts)
    if as_rows:
        blocks = [x1, x1, x2, x2, x1, x3, x2, x3, squares, ones]
    else:
        blocks = [x1, x2, x1, x2, x3, x1, x3, x2, ones, squares]
    return jnp.concatenate(blocks + [zeros] * 6, axis=0)


def stack_values(values, stack):
    groups = values.shape[0] // LANES
    low = lane_of((LANES, LANES)) < HALF
    for group in range(groups):
        rows = values[group * LANES : (group + 1) * LANES]
        turned = pltpu.roll(rows, HALF, 1)
        for h in range(2):
            top = jnp.where(low, turned if h else rows, 0.0)
            bottom = jnp.where(low, 0.0, rows if h else turned)
            high, rest = two_parts(jnp.concatenate([top, bottom], axis=0))
            stack[h * groups + group, :, :LANES] = high
            stack[h * groups + group, :, LANES:] = rest


def fill_left(out_pts, left):
    for start in range(0, left.shape[0], LANES):
        piece = augmented(out_pts[:, start : start + LANES], True)
        left[start : start + LANES] = piece.T.astype(BF16)


def fill_right(in_pts, right):
    for start in range(0, right.shape[1], 256):
        right[:, start : start + 256] = augmented(in_pts[:, start : start + 256], False).astype(BF16)


def apply_kernel_matrix(left, right, stack, result):
    outs, ins = left.shape[0], right.shape[1]
    result[...] = jnp.zeros_like(result)
    tile = min(512, outs // 2)
    pairs = ins // 256

    def step(index, carry):
        at = pl.multiple_of(lax.div(index, pairs) * tile, tile)
        pair = lax.rem(index, pairs)
        columns = right[:, pl.ds(pl.multiple_of(pair * 256, 256), 256)]
        halves = []
        for h in range(2):
            lines = left[pl.ds(h * (outs // 2) + at, tile)]
            halves.append(two_parts(jnp.exp(bf16_dot(lines, columns, 1, 0))))
        total = result[pl.ds(at, tile)]
        for a in range(2):
            cut = slice(a * LANES, (a + 1) * LANES)
            high, low = (
                jnp.concatenate([halves[0][part][:, cut], halves[1][part][:, cut]], axis=1) for part in range(2)
            )
            weights = stack[pair * 2 + a]
            both = bf16_dot(high, weights, 1, 0)
            total = total + both[:, :LANES] + both[:, LANES:]
            total = total + bf16_dot(low, weights[:, :LANES], 1, 0)
        result[pl.ds(at, tile)] = total
        return carry

    lax.fori_loop(0, (outs // 2 // tile) * pairs, step, 0)


def first_product_kernel(row_ref, col_ref, rhs_ref, out_ref, left, right, stack, result):
    fill_left(ordered(row_ref), left)
    fill_right(ordered(col_ref), right)
    stack_values(rhs_ref[...], stack)
    apply_kernel_matrix(left, right, stack, result)
    for place in range(out_ref.shape[0]):
        out_ref[place] = result[place * 32 : place * 32 + 32]


def second_product_kernel(
    row_ref, col_ref, raw_ref, rhs_ref, noise_ref, out_ref, image_ref, left, right, stack, result, grams
):
    rhs = rhs_ref[...]
    image = raw_ref[...] + noise_ref[...] * rhs
    image_ref[...] = image
    fill_left(ordered(row_ref), left)
    fill_right(ordered(col_ref), right)
    stack_values(rhs - THETA * image, stack)
    apply_kernel_matrix(left, right, stack, result)
    gram = gram_of(joined(two_parts(rhs), two_parts(image)))
    grams[0:32] = folded(summed_halves(gram[:LANES, :LANES]))
    grams[32:64] = folded(summed_halves(gram[:LANES, LANES:]))
    grams[64:96] = folded(summed_halves(gram[LANES:, LANES:]))
    own = lax.axis_index(COL)
    lines = [grams[pl.ds(32 * m + own, 1)] for m in range(3)]
    tail = jnp.concatenate(lines + [jnp.zeros((1, LANES), F32)], axis=0)
    for place in range(out_ref.shape[0]):
        for quad in range(8):
            start = place * 32 + quad * 4
            out_ref[place, quad] = result[start : start + 4]
        out_ref[place, 8] = tail


def product_cost(outs, ins):
    return pl.CostEstimate(
        flops=2 * outs * ins * 512, bytes_accessed=8 * (outs + ins) * HALF, transcendentals=outs * ins
    )


def product_scratch(outs, ins):
    return [
        pltpu.VMEM((outs, LANES), BF16),
        pltpu.VMEM((LANES, ins), BF16),
        pltpu.VMEM((ins // LANES, 256, 256), BF16),
        pltpu.VMEM((outs // 2, LANES), F32),
    ]


def first_product(row_pts, col_pts, rhs):
    outs, ins = row_pts.shape[0] * 64, col_pts.shape[0] * 64
    return pl.pallas_call(
        first_product_kernel,
        in_specs=[VMEM] * 3,
        out_specs=VMEM,
        out_shape=jax.ShapeDtypeStruct((row_pts.shape[0], 32, LANES), F32),
        scratch_shapes=product_scratch(outs, ins),
        cost_estimate=product_cost(outs, ins),
        compiler_params=PARAMS,
        name="first_product",
    )(row_pts, col_pts, rhs)


def second_product(row_pts, col_pts, raw, rhs, noise):
    outs, ins = row_pts.shape[0] * 64, col_pts.shape[0] * 64
    return pl.pallas_call(
        second_product_kernel,
        in_specs=[VMEM] * 5,
        out_specs=[VMEM] * 2,
        out_shape=[
            jax.ShapeDtypeStruct((row_pts.shape[0], 9, 4, LANES), F32),
            jax.ShapeDtypeStruct((ins // 2, LANES), F32),
        ],
        scratch_shapes=product_scratch(outs, ins) + [pltpu.VMEM((96, LANES), F32)],
        cost_estimate=product_cost(outs, ins),
        compiler_params=PARAMS,
        name="second_product",
    )(row_pts, col_pts, raw, rhs, noise)


def two_parts(value):
    high = value.astype(BF16)
    return high, (value - high.astype(F32)).astype(BF16)


def bf16_dot(first, second, first_dim, second_dim):
    dims = (((first_dim,), (second_dim,)), ((), ()))
    return lax.dot_general(first, second, dims, preferred_element_type=F32)


def parts_dot(first, second, first_dim=1, second_dim=0):
    high = bf16_dot(first[0], second[0], first_dim, second_dim)
    cross = bf16_dot(first[0], second[1], first_dim, second_dim)
    return high + cross + bf16_dot(first[1], second[0], first_dim, second_dim)


def gram_of(parts):
    high = bf16_dot(parts[0], parts[0], 0, 0)
    cross = bf16_dot(parts[0], parts[1], 0, 0)
    return high + cross + cross.T


def joined(*pairs):
    return tuple(jnp.concatenate([pair[i] for pair in pairs], axis=1) for i in range(2))


def summed_halves(gram):
    return gram[:HALF, :HALF] + gram[HALF:, HALF:]


def folded(square):
    return jnp.concatenate([square[:32], square[32:]], axis=1)


def unfolded(lines):
    return jnp.concatenate([lines[:, :HALF], lines[:, HALF:]], axis=0)


def row_and_column():
    shape = (HALF, HALF)
    return lax.broadcasted_iota(jnp.int32, shape, 0), lax.broadcasted_iota(jnp.int32, shape, 1)


def squares_of(first, second, third):
    row, column = row_and_column()
    diagonal = jnp.sum(jnp.where(row == column, second, 0.0), axis=0, keepdims=True)
    under = jnp.where(row == HALF - 1, diagonal, jnp.where(row == HALF - 2, diagonal[:, HALF - 1 :], 0.0))
    return jnp.where(column >= row, first, second), jnp.where(column >= row, third, under)


def matrices_of(upper, lower):
    row, column = row_and_column()
    turned, beneath = upper.T, lower.T
    diagonal = jnp.where(column == HALF - 1, lower[HALF - 2 : HALF - 1, :1], lower[HALF - 1 :])
    first = jnp.where(column >= row, upper, turned)
    second = jnp.where(column == row, diagonal, jnp.where(column < row, upper, turned))
    return first, second, jnp.where(column >= row, lower, beneath)


def small_dot(first, second):
    return jnp.dot(first, second, precision=HIGH, preferred_element_type=F32)


def twice(coefs):
    zero = jnp.zeros_like(coefs)
    return jnp.concatenate(
        [jnp.concatenate([coefs, zero], axis=1), jnp.concatenate([zero, coefs], axis=1)], axis=0
    )


def line(tile, index):
    return jnp.broadcast_to(tile[index : index + 1], tile.shape)


def solve_sym(*systems):
    sub = lax.broadcasted_iota(jnp.int32, (8, LANES), 0)
    state = []
    for matrix, target in systems:
        both = jnp.concatenate([0.5 * (matrix + matrix.T), target], axis=1)
        state.append(tuple(both[8 * t : 8 * t + 8] for t in range(8)))

    def step(group, state):
        state = [list(tiles) for tiles in state]
        for quad in range(2):
            lanes = [jnp.full((8, LANES), group * 8 + quad * 4 + j, jnp.int32) for j in range(4)]
            spread = [
                [[jnp.take_along_axis(tile, lane, axis=1) for tile in tiles] for lane in lanes] for tiles in state
            ]
            for j in range(4):
                at = quad * 4 + j
                here = sub == at
                for tiles, columns in zip(state, spread):
                    inverse = 1.0 / line(columns[j][0], at)
                    row = line(tiles[0], at) * inverse
                    for t in range(8):
                        new = tiles[t] - columns[j][t] * row
                        tiles[t] = jnp.where(here, row, new) if t == 0 else new
                    for later in range(j + 1, 4):
                        ratio = line(columns[later][0], at) * inverse
                        for t in range(8):
                            new = columns[later][t] - columns[j][t] * ratio
                            columns[later][t] = jnp.where(here, ratio, new) if t == 0 else new
        return tuple(tuple(tiles[1:] + tiles[:1]) for tiles in state)

    state = lax.fori_loop(0, 8, step, tuple(state))
    return [jnp.concatenate(tiles, axis=0)[:, HALF:] for tiles in state]


def middle_kernel(unit_ref, rhs_ref, image_ref, noise_ref, share_ref, second_ref, coef_ref, lines):
    for place in range(unit_ref.shape[0]):
        tail = unit_ref[place, 8]
        for m in range(3):
            lines[32 * m + place : 32 * m + place + 1] = tail[m : m + 1]
    gram, curv, square = (unfolded(lines[32 * m : 32 * m + 32]) for m in range(3))
    row, column = row_and_column()
    eye = jnp.where(row == column, 1.0, 0.0)
    coef0, inverse = solve_sym((curv, gram), (gram, eye))
    cross = small_dot(curv, coef0)
    gram1 = gram - cross - cross.T + small_dot(coef0.T, small_dot(square, coef0))
    dcoef = small_dot(inverse, gram1)
    rhs, image = rhs_ref[...], image_ref[...]
    raw = jnp.concatenate([unit_ref[i, quad] for i in range(unit_ref.shape[0]) for quad in range(8)], axis=0)
    second = raw + noise_ref[...] * (rhs - THETA * image)
    second_ref[...] = second
    scaled = coef0 * (1.0 / THETA)
    down = -twice(coef0)
    turn = twice(dcoef)
    mix = jnp.concatenate(
        [
            jnp.concatenate([turn, jnp.zeros_like(turn)], axis=1),
            jnp.concatenate([down, down], axis=1),
        ],
        axis=0,
    )
    mix1 = jnp.concatenate([twice(eye - scaled + dcoef), twice(scaled)], axis=0)
    rhs_parts, image_parts = two_parts(rhs), two_parts(image)
    change = parts_dot(joined(rhs_parts, image_parts), two_parts(mix))
    direction, residual = rhs + change[:, :LANES], rhs + change[:, LANES:]
    image1 = two_parts(parts_dot(joined(image_parts, two_parts(second)), two_parts(mix1)))
    crossed = parts_dot(joined(two_parts(direction), image1), image1, 0, 0)
    curv1 = summed_halves(crossed[:LANES])
    upper, lower = squares_of(
        0.5 * (curv1 + curv1.T),
        summed_halves(gram_of(two_parts(residual))),
        summed_halves(crossed[LANES:]),
    )
    lines[0:32] = folded(upper)
    lines[32:64] = folded(lower)
    start = pl.multiple_of(lax.axis_index(COL[-1]) * 16, 16)
    part = jnp.concatenate([lines[pl.ds(32 * m + start, 16)] for m in range(2)], axis=0)
    for place in range(share_ref.shape[0]):
        share_ref[place] = part
    coef_ref[0:64] = jnp.concatenate([coef0, dcoef], axis=1)
    coef_ref[64:128] = jnp.concatenate([gram, eye], axis=1)


def middle(units, rhs, image, noise, rows):
    return pl.pallas_call(
        middle_kernel,
        in_specs=[VMEM] * 4,
        out_specs=[VMEM] * 3,
        out_shape=[
            jax.ShapeDtypeStruct((rows, 32, LANES), F32),
            jax.ShapeDtypeStruct(rhs.shape, F32),
            jax.ShapeDtypeStruct((128, LANES), F32),
        ],
        scratch_shapes=[pltpu.VMEM((96, LANES), F32)],
        compiler_params=PARAMS,
        name="middle",
    )(units, rhs, image, noise)


def final_kernel(lines_ref, coef_ref, rhs_ref, packed_ref, image_ref, second_ref, sol_ref, res_ref, norm_ref):
    low = lane_of((32, LANES)) < HALF
    upper, lower = (
        unfolded(jnp.concatenate([lines_ref[half, 16 * m : 16 * m + 16] for half in range(2)], axis=0))
        for m in range(2)
    )
    curv1, gram1, square = matrices_of(upper, lower)
    coef0, dcoef = coef_ref[0:64, :HALF], coef_ref[0:64, HALF:]
    gram, eye = coef_ref[64:128, :HALF], coef_ref[64:128, HALF:]
    (coef1,) = solve_sym((curv1, gram1))
    cross = small_dot(curv1, coef1)
    gram2 = gram1 - cross - cross.T + small_dot(coef1.T, small_dot(square, coef1))
    norms = jnp.sum(eye * gram2, axis=0, keepdims=True) / jnp.sum(eye * gram, axis=0, keepdims=True)
    norm_ref[...] = jnp.sqrt(jnp.maximum(norms, 0.0))
    linear = coef0 + coef1 + small_dot(dcoef, coef1)
    quadratic = small_dot(coef0, coef1)
    scaled = quadratic * (1.0 / THETA)

    def doubled(first, second):
        first, second = first.T, second.T
        high, rest = two_parts(jnp.concatenate([first, first, second, second], axis=1))
        return jnp.concatenate([high, rest], axis=0)

    sol_c = doubled(linear, -quadratic)
    res_c = doubled(linear - scaled, scaled)

    def spread(ref, start):
        pieces = []
        for part in range(4):
            rows = ref[start // 2 + part * 32 : start // 2 + part * 32 + 32]
            pieces += [jnp.where(low, rows, 0.0), jnp.where(low, 0.0, rows)]
        return two_parts(jnp.concatenate(pieces, axis=0))

    def mixed(coefs, pair):
        both = bf16_dot(coefs, pair[0], 1, 1)
        return both[:HALF] + both[HALF:] + bf16_dot(coefs[:HALF], pair[1], 1, 1)

    for start in range(0, rhs_ref.shape[1], 256):
        cut = slice(start, start + 256)
        image = spread(image_ref, start)
        sol_ref[:, cut] = mixed(sol_c, joined(spread(packed_ref, start), image))
        res_ref[:, cut] = rhs_ref[:, cut] - mixed(res_c, joined(image, spread(second_ref, start)))


def final_outputs(lines, coefs, right_sides, rhs, image, second):
    return pl.pallas_call(
        final_kernel,
        in_specs=[VMEM] * 6,
        out_specs=[VMEM] * 3,
        out_shape=[jax.ShapeDtypeStruct(right_sides.shape, F32)] * 2
        + [jax.ShapeDtypeStruct((1, HALF), F32)],
        compiler_params=PARAMS,
        name="final_outputs",
    )(lines, coefs, right_sides, rhs, image, second)


def exchanged(parts, axis):
    return lax.all_to_all(parts, axis, 0, 0, tiled=True)


def shared(value, axis):
    return exchanged(jnp.broadcast_to(value[None], (lax.axis_size(axis), *value.shape)), axis)


def on_device(points, noise_level, right_sides):
    rows, cols = lax.axis_size("row"), lax.axis_size(COL)
    row_units, col_units = own_units(points, rows, cols)
    col_pts = exchanged(col_units, COL)
    row_pts = exchanged(row_units, "row")
    rhs, noise = prepare(right_sides, noise_level)

    part = first_product(row_pts, col_pts, rhs)
    own = jnp.sum(exchanged(part, "row"), axis=0)
    raw = shared(own, COL).reshape(-1, LANES)
    part, image = second_product(row_pts, col_pts, raw, rhs, noise)
    own = jnp.sum(exchanged(part, "row"), axis=0)
    share, second, coefs = middle(shared(own, COL), rhs, image, noise, rows)
    lines = lax.all_gather(jnp.sum(exchanged(share, "row"), axis=0), COL[-1])
    sol, res, norms = final_outputs(lines, coefs, right_sides, rhs, image, second)
    return sol, res, norms[0]


def solution(mesh):
    torus = Mesh(
        mesh.devices.reshape(mesh.shape["row"], 4, 4, 2), ("row", "col_0", "col_1", "col_2")
    )
    return jax.shard_map(
        on_device,
        mesh=torus,
        in_specs=(P(None, ROW_COL), P("row"), P(None, "row")),
        out_specs=(P(None, "row"), P(None, "row"), P()),
        check_vma=False,
    )
```

```python
import jax
import jax.numpy as jnp
from jax import lax
from jax.experimental import pallas as pl
from jax.experimental.pallas import tpu as pltpu
from jax.sharding import Mesh
from jax.sharding import PartitionSpec as P

COL = ("col_0", "col_1", "col_2")
ROW_COL = ("row", "col_0", "col_1", "col_2")
HIGH = lax.Precision.HIGHEST
F32 = jnp.float32
BF16 = jnp.bfloat16
THETA = 0.5
LANES = 128
HALF = 64
VMEM = pl.BlockSpec(memory_space=pltpu.VMEM)
PARAMS = pltpu.CompilerParams(vmem_limit_bytes=16 * 1024 * 1024)


def lane_of(shape):
    return lax.broadcasted_iota(jnp.int32, shape, len(shape) - 1)


def packed(turned):
    return jnp.concatenate([turned[:32], turned[32:64]], axis=1)


def own_units(points, rows, cols):
    unit = jnp.concatenate([points[:4], points[4:]], axis=1)
    return (jnp.broadcast_to(unit[None], (count, 4, LANES)) for count in (rows, cols))


def prepare_kernel(rhs_ref, noise_ref, packed_out, noise_out):
    low = lane_of((32, LANES)) < HALF
    for tile in range(rhs_ref.shape[1] // LANES):
        turned = rhs_ref[:, tile * LANES : (tile + 1) * LANES].T
        noise = noise_ref[:, tile * LANES : (tile + 1) * LANES]
        noise = jnp.broadcast_to(noise, (LANES, LANES)).T
        for part in range(2):
            rows = slice(tile * 64 + part * 32, tile * 64 + part * 32 + 32)
            packed_out[rows] = packed(turned[part * 64 : part * 64 + 64])
            noise_out[rows] = jnp.where(
                low, noise[part * 64 : part * 64 + 32], noise[part * 64 + 32 : part * 64 + 64]
            )


def prepare(right_sides, noise_level):
    ins = right_sides.shape[1]
    return pl.pallas_call(
        prepare_kernel,
        in_specs=[VMEM] * 2,
        out_specs=[VMEM] * 2,
        out_shape=[jax.ShapeDtypeStruct((ins // 2, LANES), F32)] * 2,
        cost_estimate=pl.CostEstimate(flops=4 * 10**9, bytes_accessed=6 * 10**6, transcendentals=0),
        compiler_params=PARAMS,
        name="prepare",
    )(right_sides, noise_level[None, :])


def ordered(ref):
    place = lane_of((8, LANES)) // 32
    low = lane_of((4, LANES)) < HALF
    units = []
    for index in range(ref.shape[0]):
        unit = ref[index]
        turned = pltpu.roll(unit, HALF, 1)
        units.append(
            jnp.concatenate([jnp.where(low, unit, turned), jnp.where(low, turned, unit)], axis=0)
        )
    pieces = []
    for h in range(2):
        for start in range(0, len(units), 4):
            piece = None
            for q in range(4):
                unit = units[start + q]
                if (q - h) % 2:
                    unit = pltpu.roll(unit, 32, 1)
                piece = unit if piece is None else jnp.where(place == q, unit, piece)
            pieces.append(piece)
    return jnp.concatenate(pieces, axis=1)


def rounded(value):
    return value.astype(BF16).astype(F32)


def three_parts(value):
    first = rounded(value)
    rest = value - first
    second = rounded(rest)
    return first, second, rest - second


def augmented(pts, as_rows):
    x1, x2, x3 = three_parts(pts)
    half_sq = -0.5 * jnp.sum(pts * pts, axis=0, keepdims=True)
    s1, s2, s3 = three_parts(half_sq)
    sub = lax.broadcasted_iota(jnp.int32, pts.shape, 0)
    squares = jnp.where(sub == 0, s1, jnp.where(sub == 1, s2, jnp.where(sub == 2, s3, 0.0)))
    ones = jnp.where(sub < 3, 1.0, 0.0)
    zeros = jnp.zeros_like(pts)
    if as_rows:
        blocks = [x1, x1, x2, x2, x1, x3, x2, x3, squares, ones]
    else:
        blocks = [x1, x2, x1, x2, x3, x1, x3, x2, ones, squares]
    return jnp.concatenate(blocks + [zeros] * 6, axis=0)


def stack_values(values, stack):
    groups = values.shape[0] // LANES
    low = lane_of((LANES, LANES)) < HALF
    for group in range(groups):
        rows = values[group * LANES : (group + 1) * LANES]
        turned = pltpu.roll(rows, HALF, 1)
        for h in range(2):
            top = jnp.where(low, turned if h else rows, 0.0)
            bottom = jnp.where(low, 0.0, rows if h else turned)
            high, rest = two_parts(jnp.concatenate([top, bottom], axis=0))
            stack[h * groups + group, :, :LANES] = high
            stack[h * groups + group, :, LANES:] = rest


def fill_left(out_pts, left):
    for start in range(0, left.shape[0], LANES):
        piece = augmented(out_pts[:, start : start + LANES], True)
        left[start : start + LANES] = piece.T.astype(BF16)


def fill_right(in_pts, right):
    for start in range(0, right.shape[1], 256):
        right[:, start : start + 256] = augmented(in_pts[:, start : start + 256], False).astype(BF16)


def apply_kernel_matrix(left, right, stack, result):
    outs, ins = left.shape[0], right.shape[1]
    result[...] = jnp.zeros_like(result)
    tile = min(512, outs // 2)
    pairs = ins // 256

    def step(index, carry):
        at = pl.multiple_of(lax.div(index, pairs) * tile, tile)
        pair = lax.rem(index, pairs)
        columns = right[:, pl.ds(pl.multiple_of(pair * 256, 256), 256)]
        halves = []
        for h in range(2):
            lines = left[pl.ds(h * (outs // 2) + at, tile)]
            halves.append(two_parts(jnp.exp(bf16_dot(lines, columns, 1, 0))))
        total = result[pl.ds(at, tile)]
        for a in range(2):
            cut = slice(a * LANES, (a + 1) * LANES)
            high, low = (
                jnp.concatenate([halves[0][part][:, cut], halves[1][part][:, cut]], axis=1) for part in range(2)
            )
            weights = stack[pair * 2 + a]
            both = bf16_dot(high, weights, 1, 0)
            total = total + both[:, :LANES] + both[:, LANES:]
            total = total + bf16_dot(low, weights[:, :LANES], 1, 0)
        result[pl.ds(at, tile)] = total
        return carry

    lax.fori_loop(0, (outs // 2 // tile) * pairs, step, 0, unroll=8)


def first_product_kernel(row_ref, col_ref, rhs_ref, out_ref, left, right, stack, result):
    fill_left(ordered(row_ref), left)
    fill_right(ordered(col_ref), right)
    stack_values(rhs_ref[...], stack)
    apply_kernel_matrix(left, right, stack, result)
    for place in range(out_ref.shape[0]):
        out_ref[place] = result[place * 32 : place * 32 + 32]


def second_product_kernel(
    row_ref, col_ref, raw_ref, rhs_ref, noise_ref, out_ref, image_ref, left, right, stack, result, grams
):
    rhs = rhs_ref[...]
    image = raw_ref[...] + noise_ref[...] * rhs
    image_ref[...] = image
    fill_left(ordered(row_ref), left)
    fill_right(ordered(col_ref), right)
    stack_values(rhs - THETA * image, stack)
    apply_kernel_matrix(left, right, stack, result)
    gram = gram_of(joined(two_parts(rhs), two_parts(image)))
    grams[0:32] = folded(summed_halves(gram[:LANES, :LANES]))
    grams[32:64] = folded(summed_halves(gram[:LANES, LANES:]))
    grams[64:96] = folded(summed_halves(gram[LANES:, LANES:]))
    own = lax.axis_index(COL)
    lines = [grams[pl.ds(32 * m + own, 1)] for m in range(3)]
    tail = jnp.concatenate(lines + [jnp.zeros((1, LANES), F32)], axis=0)
    for place in range(out_ref.shape[0]):
        for quad in range(8):
            start = place * 32 + quad * 4
            out_ref[place, quad] = result[start : start + 4]
        out_ref[place, 8] = tail


def product_cost(outs, ins):
    return pl.CostEstimate(
        flops=2 * outs * ins * 512, bytes_accessed=8 * (outs + ins) * HALF, transcendentals=outs * ins
    )


def product_scratch(outs, ins):
    return [
        pltpu.VMEM((outs, LANES), BF16),
        pltpu.VMEM((LANES, ins), BF16),
        pltpu.VMEM((ins // LANES, 256, 256), BF16),
        pltpu.VMEM((outs // 2, LANES), F32),
    ]


def first_product(row_pts, col_pts, rhs):
    outs, ins = row_pts.shape[0] * 64, col_pts.shape[0] * 64
    return pl.pallas_call(
        first_product_kernel,
        in_specs=[VMEM] * 3,
        out_specs=VMEM,
        out_shape=jax.ShapeDtypeStruct((row_pts.shape[0], 32, LANES), F32),
        scratch_shapes=product_scratch(outs, ins),
        cost_estimate=product_cost(outs, ins),
        compiler_params=PARAMS,
        name="first_product",
    )(row_pts, col_pts, rhs)


def second_product(row_pts, col_pts, raw, rhs, noise):
    outs, ins = row_pts.shape[0] * 64, col_pts.shape[0] * 64
    return pl.pallas_call(
        second_product_kernel,
        in_specs=[VMEM] * 5,
        out_specs=[VMEM] * 2,
        out_shape=[
            jax.ShapeDtypeStruct((row_pts.shape[0], 9, 4, LANES), F32),
            jax.ShapeDtypeStruct((ins // 2, LANES), F32),
        ],
        scratch_shapes=product_scratch(outs, ins) + [pltpu.VMEM((96, LANES), F32)],
        cost_estimate=product_cost(outs, ins),
        compiler_params=PARAMS,
        name="second_product",
    )(row_pts, col_pts, raw, rhs, noise)


def two_parts(value):
    high = value.astype(BF16)
    return high, (value - high.astype(F32)).astype(BF16)


def bf16_dot(first, second, first_dim, second_dim):
    dims = (((first_dim,), (second_dim,)), ((), ()))
    return lax.dot_general(first, second, dims, preferred_element_type=F32)


def parts_dot(first, second, first_dim=1, second_dim=0):
    high = bf16_dot(first[0], second[0], first_dim, second_dim)
    cross = bf16_dot(first[0], second[1], first_dim, second_dim)
    return high + cross + bf16_dot(first[1], second[0], first_dim, second_dim)


def gram_of(parts):
    high = bf16_dot(parts[0], parts[0], 0, 0)
    cross = bf16_dot(parts[0], parts[1], 0, 0)
    return high + cross + cross.T


def joined(*pairs):
    return tuple(jnp.concatenate([pair[i] for pair in pairs], axis=1) for i in range(2))


def summed_halves(gram):
    return gram[:HALF, :HALF] + gram[HALF:, HALF:]


def folded(square):
    return jnp.concatenate([square[:32], square[32:]], axis=1)


def unfolded(lines):
    return jnp.concatenate([lines[:, :HALF], lines[:, HALF:]], axis=0)


def row_and_column():
    shape = (HALF, HALF)
    return lax.broadcasted_iota(jnp.int32, shape, 0), lax.broadcasted_iota(jnp.int32, shape, 1)


def squares_of(first, second, third):
    row, column = row_and_column()
    diagonal = jnp.sum(jnp.where(row == column, second, 0.0), axis=0, keepdims=True)
    under = jnp.where(row == HALF - 1, diagonal, jnp.where(row == HALF - 2, diagonal[:, HALF - 1 :], 0.0))
    return jnp.where(column >= row, first, second), jnp.where(column >= row, third, under)


def matrices_of(upper, lower):
    row, column = row_and_column()
    turned, beneath = upper.T, lower.T
    diagonal = jnp.where(column == HALF - 1, lower[HALF - 2 : HALF - 1, :1], lower[HALF - 1 :])
    first = jnp.where(column >= row, upper, turned)
    second = jnp.where(column == row, diagonal, jnp.where(column < row, upper, turned))
    return first, second, jnp.where(column >= row, lower, beneath)


def small_dot(first, second):
    return jnp.dot(first, second, precision=HIGH, preferred_element_type=F32)


def twice(coefs):
    zero = jnp.zeros_like(coefs)
    return jnp.concatenate(
        [jnp.concatenate([coefs, zero], axis=1), jnp.concatenate([zero, coefs], axis=1)], axis=0
    )


def line(tile, index):
    return jnp.broadcast_to(tile[index : index + 1], tile.shape)


def solve_sym(*systems):
    sub = lax.broadcasted_iota(jnp.int32, (8, LANES), 0)
    state = []
    for matrix, target in systems:
        both = jnp.concatenate([0.5 * (matrix + matrix.T), target], axis=1)
        state.append(tuple(both[8 * t : 8 * t + 8] for t in range(8)))

    def step(group, state):
        state = [list(tiles) for tiles in state]
        for quad in range(1):
            lanes = [jnp.full((8, LANES), group * 8 + j, jnp.int32) for j in range(8)]
            spread = [
                [[jnp.take_along_axis(tile, lane, axis=1) for tile in tiles] for lane in lanes] for tiles in state
            ]
            for j in range(8):
                at = j
                here = sub == at
                for tiles, columns in zip(state, spread):
                    inverse = 1.0 / line(columns[j][0], at)
                    row = line(tiles[0], at) * inverse
                    for t in range(8):
                        new = tiles[t] - columns[j][t] * row
                        tiles[t] = jnp.where(here, row, new) if t == 0 else new
                    for later in range(j + 1, 8):
                        ratio = line(columns[later][0], at) * inverse
                        for t in range(8):
                            new = columns[later][t] - columns[j][t] * ratio
                            columns[later][t] = jnp.where(here, ratio, new) if t == 0 else new
        return tuple(tuple(tiles[1:] + tiles[:1]) for tiles in state)

    state = lax.fori_loop(0, 8, step, tuple(state))
    return [jnp.concatenate(tiles, axis=0)[:, HALF:] for tiles in state]


def middle_kernel(unit_ref, rhs_ref, image_ref, noise_ref, share_ref, second_ref, coef_ref, lines):
    for place in range(unit_ref.shape[0]):
        tail = unit_ref[place, 8]
        for m in range(3):
            lines[32 * m + place : 32 * m + place + 1] = tail[m : m + 1]
    gram, curv, square = (unfolded(lines[32 * m : 32 * m + 32]) for m in range(3))
    row, column = row_and_column()
    eye = jnp.where(row == column, 1.0, 0.0)
    coef0, inverse = solve_sym((curv, gram), (gram, eye))
    cross = small_dot(curv, coef0)
    gram1 = gram - cross - cross.T + small_dot(coef0.T, small_dot(square, coef0))
    dcoef = small_dot(inverse, gram1)
    rhs, image = rhs_ref[...], image_ref[...]
    raw = jnp.concatenate([unit_ref[i, quad] for i in range(unit_ref.shape[0]) for quad in range(8)], axis=0)
    second = raw + noise_ref[...] * (rhs - THETA * image)
    second_ref[...] = second
    scaled = coef0 * (1.0 / THETA)
    down = -twice(coef0)
    turn = twice(dcoef)
    mix = jnp.concatenate(
        [
            jnp.concatenate([turn, jnp.zeros_like(turn)], axis=1),
            jnp.concatenate([down, down], axis=1),
        ],
        axis=0,
    )
    mix1 = jnp.concatenate([twice(eye - scaled + dcoef), twice(scaled)], axis=0)
    rhs_parts, image_parts = two_parts(rhs), two_parts(image)
    change = parts_dot(joined(rhs_parts, image_parts), two_parts(mix))
    direction, residual = rhs + change[:, :LANES], rhs + change[:, LANES:]
    image1 = two_parts(parts_dot(joined(image_parts, two_parts(second)), two_parts(mix1)))
    crossed = parts_dot(joined(two_parts(direction), image1), image1, 0, 0)
    curv1 = summed_halves(crossed[:LANES])
    upper, lower = squares_of(
        0.5 * (curv1 + curv1.T),
        summed_halves(gram_of(two_parts(residual))),
        summed_halves(crossed[LANES:]),
    )
    lines[0:32] = folded(upper)
    lines[32:64] = folded(lower)
    start = pl.multiple_of(lax.axis_index(COL[-1]) * 16, 16)
    part = jnp.concatenate([lines[pl.ds(32 * m + start, 16)] for m in range(2)], axis=0)
    for place in range(share_ref.shape[0]):
        share_ref[place] = part
    coef_ref[0:64] = jnp.concatenate([coef0, dcoef], axis=1)
    coef_ref[64:128] = jnp.concatenate([gram, eye], axis=1)


def middle(units, rhs, image, noise, rows):
    return pl.pallas_call(
        middle_kernel,
        in_specs=[VMEM] * 4,
        out_specs=[VMEM] * 3,
        out_shape=[
            jax.ShapeDtypeStruct((rows, 32, LANES), F32),
            jax.ShapeDtypeStruct(rhs.shape, F32),
            jax.ShapeDtypeStruct((128, LANES), F32),
        ],
        scratch_shapes=[pltpu.VMEM((96, LANES), F32)],
        compiler_params=PARAMS,
        name="middle",
    )(units, rhs, image, noise)


def final_kernel(lines_ref, coef_ref, rhs_ref, packed_ref, image_ref, second_ref, sol_ref, res_ref, norm_ref):
    low = lane_of((32, LANES)) < HALF
    upper, lower = (
        unfolded(jnp.concatenate([lines_ref[half, 16 * m : 16 * m + 16] for half in range(2)], axis=0))
        for m in range(2)
    )
    curv1, gram1, square = matrices_of(upper, lower)
    coef0, dcoef = coef_ref[0:64, :HALF], coef_ref[0:64, HALF:]
    gram, eye = coef_ref[64:128, :HALF], coef_ref[64:128, HALF:]
    (coef1,) = solve_sym((curv1, gram1))
    cross = small_dot(curv1, coef1)
    gram2 = gram1 - cross - cross.T + small_dot(coef1.T, small_dot(square, coef1))
    norms = jnp.sum(eye * gram2, axis=0, keepdims=True) / jnp.sum(eye * gram, axis=0, keepdims=True)
    norm_ref[...] = jnp.sqrt(jnp.maximum(norms, 0.0))
    linear = coef0 + coef1 + small_dot(dcoef, coef1)
    quadratic = small_dot(coef0, coef1)
    scaled = quadratic * (1.0 / THETA)

    def doubled(first, second):
        first, second = first.T, second.T
        high, rest = two_parts(jnp.concatenate([first, first, second, second], axis=1))
        return jnp.concatenate([high, rest], axis=0)

    sol_c = doubled(linear, -quadratic)
    res_c = doubled(linear - scaled, scaled)

    def spread(ref, start):
        pieces = []
        for part in range(4):
            rows = ref[start // 2 + part * 32 : start // 2 + part * 32 + 32]
            pieces += [jnp.where(low, rows, 0.0), jnp.where(low, 0.0, rows)]
        return two_parts(jnp.concatenate(pieces, axis=0))

    def mixed(coefs, pair):
        both = bf16_dot(coefs, pair[0], 1, 1)
        return both[:HALF] + both[HALF:] + bf16_dot(coefs[:HALF], pair[1], 1, 1)

    for start in range(0, rhs_ref.shape[1], 256):
        cut = slice(start, start + 256)
        image = spread(image_ref, start)
        sol_ref[:, cut] = mixed(sol_c, joined(spread(packed_ref, start), image))
        res_ref[:, cut] = rhs_ref[:, cut] - mixed(res_c, joined(image, spread(second_ref, start)))


def final_outputs(lines, coefs, right_sides, rhs, image, second):
    return pl.pallas_call(
        final_kernel,
        in_specs=[VMEM] * 6,
        out_specs=[VMEM] * 3,
        out_shape=[jax.ShapeDtypeStruct(right_sides.shape, F32)] * 2
        + [jax.ShapeDtypeStruct((1, HALF), F32)],
        compiler_params=PARAMS,
        name="final_outputs",
    )(lines, coefs, right_sides, rhs, image, second)


def exchanged(parts, axis):
    return lax.all_to_all(parts, axis, 0, 0, tiled=True)


def shared(value, axis):
    return exchanged(jnp.broadcast_to(value[None], (lax.axis_size(axis), *value.shape)), axis)


def on_device(points, noise_level, right_sides):
    rows, cols = lax.axis_size("row"), lax.axis_size(COL)
    row_units, col_units = own_units(points, rows, cols)
    col_pts = exchanged(col_units, COL)
    row_pts = exchanged(row_units, "row")
    rhs, noise = prepare(right_sides, noise_level)

    part = first_product(row_pts, col_pts, rhs)
    own = jnp.sum(exchanged(part, "row"), axis=0)
    raw = shared(own, COL).reshape(-1, LANES)
    part, image = second_product(row_pts, col_pts, raw, rhs, noise)
    own = jnp.sum(exchanged(part, "row"), axis=0)
    share, second, coefs = middle(shared(own, COL), rhs, image, noise, rows)
    lines = lax.all_gather(jnp.sum(exchanged(share, "row"), axis=0), COL[-1])
    sol, res, norms = final_outputs(lines, coefs, right_sides, rhs, image, second)
    return sol, res, norms[0]


def solution(mesh):
    torus = Mesh(
        mesh.devices.reshape(mesh.shape["row"], 4, 4, 2), ("row", "col_0", "col_1", "col_2")
    )
    return jax.shard_map(
        on_device,
        mesh=torus,
        in_specs=(P(None, ROW_COL), P("row"), P(None, "row")),
        out_specs=(P(None, "row"), P(None, "row"), P()),
        check_vma=False,
    )
```

```python
import jax
import jax.numpy as jnp
from jax import lax
from jax.experimental import pallas as pl
from jax.experimental.pallas import tpu as pltpu
from jax.sharding import Mesh
from jax.sharding import PartitionSpec as P

COL = ("col_0", "col_1", "col_2")
ROW_COL = ("row", "col_0", "col_1", "col_2")
HIGH = lax.Precision.HIGHEST
F32 = jnp.float32
BF16 = jnp.bfloat16
THETA = 0.5
LANES = 128
HALF = 64
VMEM = pl.BlockSpec(memory_space=pltpu.VMEM)
PARAMS = pltpu.CompilerParams(vmem_limit_bytes=16 * 1024 * 1024)


def lane_of(shape):
    return lax.broadcasted_iota(jnp.int32, shape, len(shape) - 1)


def packed(turned):
    return jnp.concatenate([turned[:32], turned[32:64]], axis=1)


def own_units(points, rows, cols):
    unit = jnp.concatenate([points[:4], points[4:]], axis=1)
    return (jnp.broadcast_to(unit[None], (count, 4, LANES)) for count in (rows, cols))


def prepare_kernel(rhs_ref, noise_ref, packed_out, noise_out):
    low = lane_of((32, LANES)) < HALF
    for tile in range(rhs_ref.shape[1] // LANES):
        turned = rhs_ref[:, tile * LANES : (tile + 1) * LANES].T
        noise = noise_ref[:, tile * LANES : (tile + 1) * LANES]
        noise = jnp.broadcast_to(noise, (LANES, LANES)).T
        for part in range(2):
            rows = slice(tile * 64 + part * 32, tile * 64 + part * 32 + 32)
            packed_out[rows] = packed(turned[part * 64 : part * 64 + 64])
            noise_out[rows] = jnp.where(
                low, noise[part * 64 : part * 64 + 32], noise[part * 64 + 32 : part * 64 + 64]
            )


def prepare(right_sides, noise_level):
    ins = right_sides.shape[1]
    return pl.pallas_call(
        prepare_kernel,
        in_specs=[VMEM] * 2,
        out_specs=[VMEM] * 2,
        out_shape=[jax.ShapeDtypeStruct((ins // 2, LANES), F32)] * 2,
        cost_estimate=pl.CostEstimate(flops=4 * 10**9, bytes_accessed=6 * 10**6, transcendentals=0),
        compiler_params=PARAMS,
        name="prepare",
    )(right_sides, noise_level[None, :])


def ordered(ref):
    place = lane_of((8, LANES)) // 32
    low = lane_of((4, LANES)) < HALF
    units = []
    for index in range(ref.shape[0]):
        unit = ref[index]
        turned = pltpu.roll(unit, HALF, 1)
        units.append(
            jnp.concatenate([jnp.where(low, unit, turned), jnp.where(low, turned, unit)], axis=0)
        )
    pieces = []
    for h in range(2):
        for start in range(0, len(units), 4):
            piece = None
            for q in range(4):
                unit = units[start + q]
                if (q - h) % 2:
                    unit = pltpu.roll(unit, 32, 1)
                piece = unit if piece is None else jnp.where(place == q, unit, piece)
            pieces.append(piece)
    return jnp.concatenate(pieces, axis=1)


def rounded(value):
    return value.astype(BF16).astype(F32)


def three_parts(value):
    first = rounded(value)
    rest = value - first
    second = rounded(rest)
    return first, second, rest - second


def augmented(pts, as_rows):
    x1, x2, x3 = three_parts(pts)
    half_sq = -0.5 * jnp.sum(pts * pts, axis=0, keepdims=True)
    s1, s2, s3 = three_parts(half_sq)
    sub = lax.broadcasted_iota(jnp.int32, pts.shape, 0)
    squares = jnp.where(sub == 0, s1, jnp.where(sub == 1, s2, jnp.where(sub == 2, s3, 0.0)))
    ones = jnp.where(sub < 3, 1.0, 0.0)
    zeros = jnp.zeros_like(pts)
    if as_rows:
        blocks = [x1, x1, x2, x2, x1, x3, x2, x3, squares, ones]
    else:
        blocks = [x1, x2, x1, x2, x3, x1, x3, x2, ones, squares]
    return jnp.concatenate(blocks + [zeros] * 6, axis=0)


def stack_values(values, stack):
    groups = values.shape[0] // LANES
    low = lane_of((LANES, LANES)) < HALF
    for group in range(groups):
        rows = values[group * LANES : (group + 1) * LANES]
        turned = pltpu.roll(rows, HALF, 1)
        for h in range(2):
            top = jnp.where(low, turned if h else rows, 0.0)
            bottom = jnp.where(low, 0.0, rows if h else turned)
            high, rest = two_parts(jnp.concatenate([top, bottom], axis=0))
            stack[h * groups + group, :, :LANES] = high
            stack[h * groups + group, :, LANES:] = rest


def fill_left(out_pts, left):
    for start in range(0, left.shape[0], LANES):
        piece = augmented(out_pts[:, start : start + LANES], True)
        left[start : start + LANES] = piece.T.astype(BF16)


def fill_right(in_pts, right):
    for start in range(0, right.shape[1], 256):
        right[:, start : start + 256] = augmented(in_pts[:, start : start + 256], False).astype(BF16)


def apply_kernel_matrix(left, right, stack, result):
    outs, ins = left.shape[0], right.shape[1]
    result[...] = jnp.zeros_like(result)
    tile = min(512, outs // 2)
    pairs = ins // 256

    def step(index, carry):
        at = pl.multiple_of(lax.div(index, pairs) * tile, tile)
        pair = lax.rem(index, pairs)
        columns = right[:, pl.ds(pl.multiple_of(pair * 256, 256), 256)]
        halves = []
        for h in range(2):
            lines = left[pl.ds(h * (outs // 2) + at, tile)]
            halves.append(two_parts(jnp.exp(bf16_dot(lines, columns, 1, 0))))
        total = result[pl.ds(at, tile)]
        for a in range(2):
            cut = slice(a * LANES, (a + 1) * LANES)
            high, low = (
                jnp.concatenate([halves[0][part][:, cut], halves[1][part][:, cut]], axis=1) for part in range(2)
            )
            weights = stack[pair * 2 + a]
            both = bf16_dot(high, weights, 1, 0)
            total = total + both[:, :LANES] + both[:, LANES:]
            total = total + bf16_dot(low, weights[:, :LANES], 1, 0)
        result[pl.ds(at, tile)] = total
        return carry

    lax.fori_loop(0, (outs // 2 // tile) * pairs, step, 0, unroll=8)


def first_product_kernel(row_ref, col_ref, rhs_ref, out_ref, left, right, stack, result):
    fill_left(ordered(row_ref), left)
    fill_right(ordered(col_ref), right)
    stack_values(rhs_ref[...], stack)
    apply_kernel_matrix(left, right, stack, result)
    for place in range(out_ref.shape[0]):
        out_ref[place] = result[place * 32 : place * 32 + 32]


def second_product_kernel(
    row_ref, col_ref, raw_ref, rhs_ref, noise_ref, out_ref, image_ref, left, right, stack, result, grams
):
    rhs = rhs_ref[...]
    image = raw_ref[...] + noise_ref[...] * rhs
    image_ref[...] = image
    fill_left(ordered(row_ref), left)
    fill_right(ordered(col_ref), right)
    stack_values(rhs - THETA * image, stack)
    apply_kernel_matrix(left, right, stack, result)
    gram = gram_of(joined(two_parts(rhs), two_parts(image)))
    grams[0:32] = folded(summed_halves(gram[:LANES, :LANES]))
    grams[32:64] = folded(summed_halves(gram[:LANES, LANES:]))
    grams[64:96] = folded(summed_halves(gram[LANES:, LANES:]))
    own = lax.axis_index(COL)
    lines = [grams[pl.ds(32 * m + own, 1)] for m in range(3)]
    tail = jnp.concatenate(lines + [jnp.zeros((1, LANES), F32)], axis=0)
    for place in range(out_ref.shape[0]):
        for quad in range(8):
            start = place * 32 + quad * 4
            out_ref[place, quad] = result[start : start + 4]
        out_ref[place, 8] = tail


def product_cost(outs, ins):
    return pl.CostEstimate(
        flops=2 * outs * ins * 512, bytes_accessed=8 * (outs + ins) * HALF, transcendentals=outs * ins
    )


def product_scratch(outs, ins):
    return [
        pltpu.VMEM((outs, LANES), BF16),
        pltpu.VMEM((LANES, ins), BF16),
        pltpu.VMEM((ins // LANES, 256, 256), BF16),
        pltpu.VMEM((outs // 2, LANES), F32),
    ]


def first_product(row_pts, col_pts, rhs):
    outs, ins = row_pts.shape[0] * 64, col_pts.shape[0] * 64
    return pl.pallas_call(
        first_product_kernel,
        in_specs=[VMEM] * 3,
        out_specs=VMEM,
        out_shape=jax.ShapeDtypeStruct((row_pts.shape[0], 32, LANES), F32),
        scratch_shapes=product_scratch(outs, ins),
        cost_estimate=product_cost(outs, ins),
        compiler_params=PARAMS,
        name="first_product",
    )(row_pts, col_pts, rhs)


def second_product(row_pts, col_pts, raw, rhs, noise):
    outs, ins = row_pts.shape[0] * 64, col_pts.shape[0] * 64
    return pl.pallas_call(
        second_product_kernel,
        in_specs=[VMEM] * 5,
        out_specs=[VMEM] * 2,
        out_shape=[
            jax.ShapeDtypeStruct((row_pts.shape[0], 9, 4, LANES), F32),
            jax.ShapeDtypeStruct((ins // 2, LANES), F32),
        ],
        scratch_shapes=product_scratch(outs, ins) + [pltpu.VMEM((96, LANES), F32)],
        cost_estimate=product_cost(outs, ins),
        compiler_params=PARAMS,
        name="second_product",
    )(row_pts, col_pts, raw, rhs, noise)


def two_parts(value):
    high = value.astype(BF16)
    return high, (value - high.astype(F32)).astype(BF16)


def bf16_dot(first, second, first_dim, second_dim):
    dims = (((first_dim,), (second_dim,)), ((), ()))
    return lax.dot_general(first, second, dims, preferred_element_type=F32)


def parts_dot(first, second, first_dim=1, second_dim=0):
    high = bf16_dot(first[0], second[0], first_dim, second_dim)
    cross = bf16_dot(first[0], second[1], first_dim, second_dim)
    return high + cross + bf16_dot(first[1], second[0], first_dim, second_dim)


def gram_of(parts):
    high = bf16_dot(parts[0], parts[0], 0, 0)
    cross = bf16_dot(parts[0], parts[1], 0, 0)
    return high + cross + cross.T


def joined(*pairs):
    return tuple(jnp.concatenate([pair[i] for pair in pairs], axis=1) for i in range(2))


def summed_halves(gram):
    return gram[:HALF, :HALF] + gram[HALF:, HALF:]


def folded(square):
    return jnp.concatenate([square[:32], square[32:]], axis=1)


def unfolded(lines):
    return jnp.concatenate([lines[:, :HALF], lines[:, HALF:]], axis=0)


def row_and_column():
    shape = (HALF, HALF)
    return lax.broadcasted_iota(jnp.int32, shape, 0), lax.broadcasted_iota(jnp.int32, shape, 1)


def squares_of(first, second, third):
    row, column = row_and_column()
    diagonal = jnp.sum(jnp.where(row == column, second, 0.0), axis=0, keepdims=True)
    under = jnp.where(row == HALF - 1, diagonal, jnp.where(row == HALF - 2, diagonal[:, HALF - 1 :], 0.0))
    return jnp.where(column >= row, first, second), jnp.where(column >= row, third, under)


def matrices_of(upper, lower):
    row, column = row_and_column()
    turned, beneath = upper.T, lower.T
    diagonal = jnp.where(column == HALF - 1, lower[HALF - 2 : HALF - 1, :1], lower[HALF - 1 :])
    first = jnp.where(column >= row, upper, turned)
    second = jnp.where(column == row, diagonal, jnp.where(column < row, upper, turned))
    return first, second, jnp.where(column >= row, lower, beneath)


def small_dot(first, second):
    return jnp.dot(first, second, precision=HIGH, preferred_element_type=F32)


def twice(coefs):
    zero = jnp.zeros_like(coefs)
    return jnp.concatenate(
        [jnp.concatenate([coefs, zero], axis=1), jnp.concatenate([zero, coefs], axis=1)], axis=0
    )


def line(tile, index):
    return jnp.broadcast_to(tile[index : index + 1], tile.shape)


def solve_sym(*systems):
    sub = lax.broadcasted_iota(jnp.int32, (8, LANES), 0)
    state = []
    for matrix, target in systems:
        both = jnp.concatenate([0.5 * (matrix + matrix.T), target], axis=1)
        state.append(tuple(both[8 * t : 8 * t + 8] for t in range(8)))

    def step(group, state):
        state = [list(tiles) for tiles in state]
        for quad in range(1):
            lanes = [jnp.full((8, LANES), group * 8 + j, jnp.int32) for j in range(8)]
            spread = [
                [[jnp.take_along_axis(tile, lane, axis=1) for tile in tiles] for lane in lanes] for tiles in state
            ]
            for j in range(8):
                at = j
                here = sub == at
                for tiles, columns in zip(state, spread):
                    inverse = 1.0 / line(columns[j][0], at)
                    row = line(tiles[0], at) * inverse
                    for t in range(8):
                        new = tiles[t] - columns[j][t] * row
                        tiles[t] = jnp.where(here, row, new) if t == 0 else new
                    for later in range(j + 1, 8):
                        ratio = line(columns[later][0], at) * inverse
                        for t in range(8):
                            new = columns[later][t] - columns[j][t] * ratio
                            columns[later][t] = jnp.where(here, ratio, new) if t == 0 else new
        return tuple(tuple(tiles[1:] + tiles[:1]) for tiles in state)

    state = lax.fori_loop(0, 8, step, tuple(state))
    return [jnp.concatenate(tiles, axis=0)[:, HALF:] for tiles in state]


def middle_kernel(unit_ref, rhs_ref, image_ref, noise_ref, share_ref, second_ref, coef_ref, lines):
    for place in range(unit_ref.shape[0]):
        tail = unit_ref[place, 8]
        for m in range(3):
            lines[32 * m + place : 32 * m + place + 1] = tail[m : m + 1]
    gram, curv, square = (unfolded(lines[32 * m : 32 * m + 32]) for m in range(3))
    row, column = row_and_column()
    eye = jnp.where(row == column, 1.0, 0.0)
    coef0, inverse = solve_sym((curv, gram), (gram, eye))
    cross = small_dot(curv, coef0)
    gram1 = gram - cross - cross.T + small_dot(coef0.T, small_dot(square, coef0))
    dcoef = small_dot(inverse, gram1)
    rhs, image = rhs_ref[...], image_ref[...]
    raw = jnp.concatenate([unit_ref[i, quad] for i in range(unit_ref.shape[0]) for quad in range(8)], axis=0)
    second = raw + noise_ref[...] * (rhs - THETA * image)
    second_ref[...] = second
    scaled = coef0 * (1.0 / THETA)
    down = -twice(coef0)
    turn = twice(dcoef)
    mix = jnp.concatenate(
        [
            jnp.concatenate([turn, jnp.zeros_like(turn)], axis=1),
            jnp.concatenate([down, down], axis=1),
        ],
        axis=0,
    )
    mix1 = jnp.concatenate([twice(eye - scaled + dcoef), twice(scaled)], axis=0)
    rhs_parts, image_parts = two_parts(rhs), two_parts(image)
    change = parts_dot(joined(rhs_parts, image_parts), two_parts(mix))
    direction, residual = rhs + change[:, :LANES], rhs + change[:, LANES:]
    image1 = two_parts(parts_dot(joined(image_parts, two_parts(second)), two_parts(mix1)))
    crossed = parts_dot(image1, joined(two_parts(direction), image1), 0, 0)
    curv1 = summed_halves(crossed[:, :LANES])
    upper, lower = squares_of(
        0.5 * (curv1 + curv1.T),
        summed_halves(gram_of(two_parts(residual))),
        summed_halves(crossed[:, LANES:]),
    )
    lines[0:32] = folded(upper)
    lines[32:64] = folded(lower)
    start = pl.multiple_of(lax.axis_index(COL[-1]) * 16, 16)
    part = jnp.concatenate([lines[pl.ds(32 * m + start, 16)] for m in range(2)], axis=0)
    for place in range(share_ref.shape[0]):
        share_ref[place] = part
    coef_ref[0:64] = jnp.concatenate([coef0, dcoef], axis=1)
    coef_ref[64:128] = jnp.concatenate([gram, eye], axis=1)


def middle(units, rhs, image, noise, rows):
    return pl.pallas_call(
        middle_kernel,
        in_specs=[VMEM] * 4,
        out_specs=[VMEM] * 3,
        out_shape=[
            jax.ShapeDtypeStruct((rows, 32, LANES), F32),
            jax.ShapeDtypeStruct(rhs.shape, F32),
            jax.ShapeDtypeStruct((128, LANES), F32),
        ],
        scratch_shapes=[pltpu.VMEM((96, LANES), F32)],
        compiler_params=PARAMS,
        name="middle",
    )(units, rhs, image, noise)


def final_kernel(lines_ref, coef_ref, rhs_ref, packed_ref, image_ref, second_ref, sol_ref, res_ref, norm_ref):
    low = lane_of((32, LANES)) < HALF
    upper, lower = (
        unfolded(jnp.concatenate([lines_ref[half, 16 * m : 16 * m + 16] for half in range(2)], axis=0))
        for m in range(2)
    )
    curv1, gram1, square = matrices_of(upper, lower)
    coef0, dcoef = coef_ref[0:64, :HALF], coef_ref[0:64, HALF:]
    gram, eye = coef_ref[64:128, :HALF], coef_ref[64:128, HALF:]
    (coef1,) = solve_sym((curv1, gram1))
    cross = small_dot(curv1, coef1)
    gram2 = gram1 - cross - cross.T + small_dot(coef1.T, small_dot(square, coef1))
    norms = jnp.sum(eye * gram2, axis=0, keepdims=True) / jnp.sum(eye * gram, axis=0, keepdims=True)
    norm_ref[...] = jnp.sqrt(jnp.maximum(norms, 0.0))
    linear = coef0 + coef1 + small_dot(dcoef, coef1)
    quadratic = small_dot(coef0, coef1)
    scaled = quadratic * (1.0 / THETA)

    def doubled(first, second):
        first, second = first.T, second.T
        high, rest = two_parts(jnp.concatenate([first, first, second, second], axis=1))
        return jnp.concatenate([high, rest], axis=0)

    sol_c = doubled(linear, -quadratic)
    res_c = doubled(linear - scaled, scaled)

    def spread(ref, start):
        pieces = []
        for part in range(4):
            rows = ref[start // 2 + part * 32 : start // 2 + part * 32 + 32]
            pieces += [jnp.where(low, rows, 0.0), jnp.where(low, 0.0, rows)]
        return two_parts(jnp.concatenate(pieces, axis=0))

    def mixed(coefs, pair):
        both = bf16_dot(coefs, pair[0], 1, 1)
        return both[:HALF] + both[HALF:] + bf16_dot(coefs[:HALF], pair[1], 1, 1)

    for start in range(0, rhs_ref.shape[1], 256):
        cut = slice(start, start + 256)
        image = spread(image_ref, start)
        sol_ref[:, cut] = mixed(sol_c, joined(spread(packed_ref, start), image))
        res_ref[:, cut] = rhs_ref[:, cut] - mixed(res_c, joined(image, spread(second_ref, start)))


def final_outputs(lines, coefs, right_sides, rhs, image, second):
    return pl.pallas_call(
        final_kernel,
        in_specs=[VMEM] * 6,
        out_specs=[VMEM] * 3,
        out_shape=[jax.ShapeDtypeStruct(right_sides.shape, F32)] * 2
        + [jax.ShapeDtypeStruct((1, HALF), F32)],
        compiler_params=PARAMS,
        name="final_outputs",
    )(lines, coefs, right_sides, rhs, image, second)


def exchanged(parts, axis):
    return lax.all_to_all(parts, axis, 0, 0, tiled=True)


def shared(value, axis):
    return exchanged(jnp.broadcast_to(value[None], (lax.axis_size(axis), *value.shape)), axis)


def on_device(points, noise_level, right_sides):
    rows, cols = lax.axis_size("row"), lax.axis_size(COL)
    row_units, col_units = own_units(points, rows, cols)
    col_pts = exchanged(col_units, COL)
    row_pts = exchanged(row_units, "row")
    rhs, noise = prepare(right_sides, noise_level)

    part = first_product(row_pts, col_pts, rhs)
    own = jnp.sum(exchanged(part, "row"), axis=0)
    raw = shared(own, COL).reshape(-1, LANES)
    part, image = second_product(row_pts, col_pts, raw, rhs, noise)
    own = jnp.sum(exchanged(part, "row"), axis=0)
    share, second, coefs = middle(shared(own, COL), rhs, image, noise, rows)
    lines = lax.all_gather(jnp.sum(exchanged(share, "row"), axis=0), COL[-1])
    sol, res, norms = final_outputs(lines, coefs, right_sides, rhs, image, second)
    return sol, res, norms[0]


def solution(mesh):
    torus = Mesh(
        mesh.devices.reshape(mesh.shape["row"], 4, 4, 2), ("row", "col_0", "col_1", "col_2")
    )
    return jax.shard_map(
        on_device,
        mesh=torus,
        in_specs=(P(None, ROW_COL), P("row"), P(None, "row")),
        out_specs=(P(None, "row"), P(None, "row"), P()),
        check_vma=False,
    )
```

```python
import jax
import jax.numpy as jnp
from jax import lax
from jax.experimental import pallas as pl
from jax.experimental.pallas import tpu as pltpu
from jax.sharding import Mesh
from jax.sharding import PartitionSpec as P

COL = ("col_0", "col_1", "col_2")
ROW_COL = ("row", "col_0", "col_1", "col_2")
HIGH = lax.Precision.HIGHEST
F32 = jnp.float32
BF16 = jnp.bfloat16
THETA = 0.5
LANES = 128
HALF = 64
VMEM = pl.BlockSpec(memory_space=pltpu.VMEM)
PARAMS = pltpu.CompilerParams(vmem_limit_bytes=16 * 1024 * 1024)


def lane_of(shape):
    return lax.broadcasted_iota(jnp.int32, shape, len(shape) - 1)


def packed(turned):
    return jnp.concatenate([turned[:32], turned[32:64]], axis=1)


def own_units(points, rows, cols):
    unit = jnp.concatenate([points[:4], points[4:]], axis=1)
    return (jnp.broadcast_to(unit[None], (count, 4, LANES)) for count in (rows, cols))


def prepare_kernel(rhs_ref, noise_ref, packed_out, noise_out):
    low = lane_of((32, LANES)) < HALF
    for tile in range(rhs_ref.shape[1] // LANES):
        turned = rhs_ref[:, tile * LANES : (tile + 1) * LANES].T
        noise = noise_ref[:, tile * LANES : (tile + 1) * LANES]
        noise = jnp.broadcast_to(noise, (LANES, LANES)).T
        for part in range(2):
            rows = slice(tile * 64 + part * 32, tile * 64 + part * 32 + 32)
            packed_out[rows] = packed(turned[part * 64 : part * 64 + 64])
            noise_out[rows] = jnp.where(
                low, noise[part * 64 : part * 64 + 32], noise[part * 64 + 32 : part * 64 + 64]
            )


def prepare(right_sides, noise_level):
    ins = right_sides.shape[1]
    return pl.pallas_call(
        prepare_kernel,
        in_specs=[VMEM] * 2,
        out_specs=[VMEM] * 2,
        out_shape=[jax.ShapeDtypeStruct((ins // 2, LANES), F32)] * 2,
        cost_estimate=pl.CostEstimate(flops=4 * 10**9, bytes_accessed=6 * 10**6, transcendentals=0),
        compiler_params=PARAMS,
        name="prepare",
    )(right_sides, noise_level[None, :])


def ordered(ref):
    place = lane_of((8, LANES)) // 32
    low = lane_of((4, LANES)) < HALF
    units = []
    for index in range(ref.shape[0]):
        unit = ref[index]
        turned = pltpu.roll(unit, HALF, 1)
        units.append(
            jnp.concatenate([jnp.where(low, unit, turned), jnp.where(low, turned, unit)], axis=0)
        )
    pieces = []
    for h in range(2):
        for start in range(0, len(units), 4):
            piece = None
            for q in range(4):
                unit = units[start + q]
                if (q - h) % 2:
                    unit = pltpu.roll(unit, 32, 1)
                piece = unit if piece is None else jnp.where(place == q, unit, piece)
            pieces.append(piece)
    return jnp.concatenate(pieces, axis=1)


def rounded(value):
    return value.astype(BF16).astype(F32)


def three_parts(value):
    first = rounded(value)
    rest = value - first
    second = rounded(rest)
    return first, second, rest - second


def augmented(pts, as_rows):
    x1, x2, x3 = three_parts(pts)
    half_sq = -0.5 * jnp.sum(pts * pts, axis=0, keepdims=True)
    s1, s2, s3 = three_parts(half_sq)
    sub = lax.broadcasted_iota(jnp.int32, pts.shape, 0)
    squares = jnp.where(sub == 0, s1, jnp.where(sub == 1, s2, jnp.where(sub == 2, s3, 0.0)))
    ones = jnp.where(sub < 3, 1.0, 0.0)
    zeros = jnp.zeros_like(pts)
    if as_rows:
        blocks = [x1, x1, x2, x2, x1, x3, x2, x3, squares, ones]
    else:
        blocks = [x1, x2, x1, x2, x3, x1, x3, x2, ones, squares]
    return jnp.concatenate(blocks + [zeros] * 6, axis=0)


def stack_values(values, stack):
    groups = values.shape[0] // LANES
    low = lane_of((LANES, LANES)) < HALF
    for group in range(groups):
        rows = values[group * LANES : (group + 1) * LANES]
        turned = pltpu.roll(rows, HALF, 1)
        for h in range(2):
            top = jnp.where(low, turned if h else rows, 0.0)
            bottom = jnp.where(low, 0.0, rows if h else turned)
            high, rest = two_parts(jnp.concatenate([top, bottom], axis=0))
            stack[h * groups + group, :, :LANES] = high
            stack[h * groups + group, :, LANES:] = rest


def fill_left(out_pts, left):
    for start in range(0, left.shape[0], LANES):
        piece = augmented(out_pts[:, start : start + LANES], True)
        left[start : start + LANES] = piece.T.astype(BF16)


def fill_right(in_pts, right):
    for start in range(0, right.shape[1], 256):
        right[:, start : start + 256] = augmented(in_pts[:, start : start + 256], False).astype(BF16)


def apply_kernel_matrix(left, right, stack, result):
    outs, ins = left.shape[0], right.shape[1]
    result[...] = jnp.zeros_like(result)
    tile = min(512, outs // 2)
    pairs = ins // 256

    def step(index, carry):
        at = pl.multiple_of(lax.div(index, pairs) * tile, tile)
        pair = lax.rem(index, pairs)
        columns = right[:, pl.ds(pl.multiple_of(pair * 256, 256), 256)]
        halves = []
        for h in range(2):
            lines = left[pl.ds(h * (outs // 2) + at, tile)]
            halves.append(two_parts(jnp.exp(bf16_dot(lines, columns, 1, 0))))
        total = result[pl.ds(at, tile)]
        for a in range(2):
            cut = slice(a * LANES, (a + 1) * LANES)
            high, low = (
                jnp.concatenate([halves[0][part][:, cut], halves[1][part][:, cut]], axis=1) for part in range(2)
            )
            weights = stack[pair * 2 + a]
            both = bf16_dot(high, weights, 1, 0)
            total = total + both[:, :LANES] + both[:, LANES:]
            total = total + bf16_dot(low, weights[:, :LANES], 1, 0)
        result[pl.ds(at, tile)] = total
        return carry

    lax.fori_loop(0, (outs // 2 // tile) * pairs, step, 0, unroll=8)


def first_product_kernel(row_ref, col_ref, rhs_ref, out_ref, left, right, stack, result):
    fill_left(ordered(row_ref), left)
    fill_right(ordered(col_ref), right)
    stack_values(rhs_ref[...], stack)
    apply_kernel_matrix(left, right, stack, result)
    for place in range(out_ref.shape[0]):
        for quad in range(8):
            start = place * 32 + quad * 4
            out_ref[place, quad] = result[start : start + 4]


def lines_of(ref):
    return jnp.concatenate([ref[i, quad] for i in range(ref.shape[0]) for quad in range(8)], axis=0)


def second_product_kernel(
    row_ref, col_ref, raw_ref, rhs_ref, noise_ref, out_ref, image_ref, left, right, stack, result, grams
):
    rhs = rhs_ref[...]
    image = lines_of(raw_ref) + noise_ref[...] * rhs
    image_ref[...] = image
    fill_left(ordered(row_ref), left)
    fill_right(ordered(col_ref), right)
    stack_values(rhs - THETA * image, stack)
    apply_kernel_matrix(left, right, stack, result)
    gram = gram_of(joined(two_parts(rhs), two_parts(image)))
    grams[0:32] = folded(summed_halves(gram[:LANES, :LANES]))
    grams[32:64] = folded(summed_halves(gram[:LANES, LANES:]))
    grams[64:96] = folded(summed_halves(gram[LANES:, LANES:]))
    own = lax.axis_index(COL)
    lines = [grams[pl.ds(32 * m + own, 1)] for m in range(3)]
    tail = jnp.concatenate(lines + [jnp.zeros((1, LANES), F32)], axis=0)
    for place in range(out_ref.shape[0]):
        for quad in range(8):
            start = place * 32 + quad * 4
            out_ref[place, quad] = result[start : start + 4]
        out_ref[place, 8] = tail


def product_cost(outs, ins):
    return pl.CostEstimate(
        flops=2 * outs * ins * 512, bytes_accessed=8 * (outs + ins) * HALF, transcendentals=outs * ins
    )


def product_scratch(outs, ins):
    return [
        pltpu.VMEM((outs, LANES), BF16),
        pltpu.VMEM((LANES, ins), BF16),
        pltpu.VMEM((ins // LANES, 256, 256), BF16),
        pltpu.VMEM((outs // 2, LANES), F32),
    ]


def first_product(row_pts, col_pts, rhs):
    outs, ins = row_pts.shape[0] * 64, col_pts.shape[0] * 64
    return pl.pallas_call(
        first_product_kernel,
        in_specs=[VMEM] * 3,
        out_specs=VMEM,
        out_shape=jax.ShapeDtypeStruct((row_pts.shape[0], 8, 4, LANES), F32),
        scratch_shapes=product_scratch(outs, ins),
        cost_estimate=product_cost(outs, ins),
        compiler_params=PARAMS,
        name="first_product",
    )(row_pts, col_pts, rhs)


def second_product(row_pts, col_pts, raw, rhs, noise):
    outs, ins = row_pts.shape[0] * 64, col_pts.shape[0] * 64
    return pl.pallas_call(
        second_product_kernel,
        in_specs=[VMEM] * 5,
        out_specs=[VMEM] * 2,
        out_shape=[
            jax.ShapeDtypeStruct((row_pts.shape[0], 9, 4, LANES), F32),
            jax.ShapeDtypeStruct((ins // 2, LANES), F32),
        ],
        scratch_shapes=product_scratch(outs, ins) + [pltpu.VMEM((96, LANES), F32)],
        cost_estimate=product_cost(outs, ins),
        compiler_params=PARAMS,
        name="second_product",
    )(row_pts, col_pts, raw, rhs, noise)


def two_parts(value):
    high = value.astype(BF16)
    return high, (value - high.astype(F32)).astype(BF16)


def bf16_dot(first, second, first_dim, second_dim):
    dims = (((first_dim,), (second_dim,)), ((), ()))
    return lax.dot_general(first, second, dims, preferred_element_type=F32)


def parts_dot(first, second, first_dim=1, second_dim=0):
    high = bf16_dot(first[0], second[0], first_dim, second_dim)
    cross = bf16_dot(first[0], second[1], first_dim, second_dim)
    return high + cross + bf16_dot(first[1], second[0], first_dim, second_dim)


def gram_of(parts):
    high = bf16_dot(parts[0], parts[0], 0, 0)
    cross = bf16_dot(parts[0], parts[1], 0, 0)
    return high + cross + cross.T


def joined(*pairs):
    return tuple(jnp.concatenate([pair[i] for pair in pairs], axis=1) for i in range(2))


def summed_halves(gram):
    return gram[:HALF, :HALF] + gram[HALF:, HALF:]


def folded(square):
    return jnp.concatenate([square[:32], square[32:]], axis=1)


def unfolded(lines):
    return jnp.concatenate([lines[:, :HALF], lines[:, HALF:]], axis=0)


def row_and_column():
    shape = (HALF, HALF)
    return lax.broadcasted_iota(jnp.int32, shape, 0), lax.broadcasted_iota(jnp.int32, shape, 1)


def squares_of(first, second, third):
    row, column = row_and_column()
    diagonal = jnp.sum(jnp.where(row == column, second, 0.0), axis=0, keepdims=True)
    under = jnp.where(row == HALF - 1, diagonal, jnp.where(row == HALF - 2, diagonal[:, HALF - 1 :], 0.0))
    return jnp.where(column >= row, first, second), jnp.where(column >= row, third, under)


def matrices_of(upper, lower):
    row, column = row_and_column()
    turned, beneath = upper.T, lower.T
    diagonal = jnp.where(column == HALF - 1, lower[HALF - 2 : HALF - 1, :1], lower[HALF - 1 :])
    first = jnp.where(column >= row, upper, turned)
    second = jnp.where(column == row, diagonal, jnp.where(column < row, upper, turned))
    return first, second, jnp.where(column >= row, lower, beneath)


def small_dot(first, second):
    return jnp.dot(first, second, precision=HIGH, preferred_element_type=F32)


def twice(coefs):
    zero = jnp.zeros_like(coefs)
    return jnp.concatenate(
        [jnp.concatenate([coefs, zero], axis=1), jnp.concatenate([zero, coefs], axis=1)], axis=0
    )


def line(tile, index):
    return jnp.broadcast_to(tile[index : index + 1], tile.shape)


def solve_sym(*systems):
    sub = lax.broadcasted_iota(jnp.int32, (8, LANES), 0)
    state = []
    for matrix, target in systems:
        both = jnp.concatenate([0.5 * (matrix + matrix.T), target], axis=1)
        state.append(tuple(both[8 * t : 8 * t + 8] for t in range(8)))

    def step(group, state):
        state = [list(tiles) for tiles in state]
        for quad in range(1):
            lanes = [jnp.full((8, LANES), group * 8 + j, jnp.int32) for j in range(8)]
            spread = [
                [[jnp.take_along_axis(tile, lane, axis=1) for tile in tiles] for lane in lanes] for tiles in state
            ]
            for j in range(8):
                at = j
                here = sub == at
                for tiles, columns in zip(state, spread):
                    inverse = 1.0 / line(columns[j][0], at)
                    row = line(tiles[0], at) * inverse
                    for t in range(8):
                        new = tiles[t] - columns[j][t] * row
                        tiles[t] = jnp.where(here, row, new) if t == 0 else new
                    for later in range(j + 1, 8):
                        ratio = line(columns[later][0], at) * inverse
                        for t in range(8):
                            new = columns[later][t] - columns[j][t] * ratio
                            columns[later][t] = jnp.where(here, ratio, new) if t == 0 else new
        return tuple(tuple(tiles[1:] + tiles[:1]) for tiles in state)

    state = lax.fori_loop(0, 8, step, tuple(state))
    return [jnp.concatenate(tiles, axis=0)[:, HALF:] for tiles in state]


def middle_kernel(unit_ref, rhs_ref, image_ref, noise_ref, share_ref, second_ref, coef_ref, lines):
    for place in range(unit_ref.shape[0]):
        tail = unit_ref[place, 8]
        for m in range(3):
            lines[32 * m + place : 32 * m + place + 1] = tail[m : m + 1]
    gram, curv, square = (unfolded(lines[32 * m : 32 * m + 32]) for m in range(3))
    row, column = row_and_column()
    eye = jnp.where(row == column, 1.0, 0.0)
    coef0, inverse = solve_sym((curv, gram), (gram, eye))
    cross = small_dot(curv, coef0)
    gram1 = gram - cross - cross.T + small_dot(coef0.T, small_dot(square, coef0))
    dcoef = small_dot(inverse, gram1)
    rhs, image = rhs_ref[...], image_ref[...]
    raw = lines_of(unit_ref)
    second = raw + noise_ref[...] * (rhs - THETA * image)
    second_ref[...] = second
    scaled = coef0 * (1.0 / THETA)
    down = -twice(coef0)
    turn = twice(dcoef)
    mix = jnp.concatenate(
        [
            jnp.concatenate([turn, jnp.zeros_like(turn)], axis=1),
            jnp.concatenate([down, down], axis=1),
        ],
        axis=0,
    )
    mix1 = jnp.concatenate([twice(eye - scaled + dcoef), twice(scaled)], axis=0)
    rhs_parts, image_parts = two_parts(rhs), two_parts(image)
    change = parts_dot(joined(rhs_parts, image_parts), two_parts(mix))
    direction, residual = rhs + change[:, :LANES], rhs + change[:, LANES:]
    image1 = two_parts(parts_dot(joined(image_parts, two_parts(second)), two_parts(mix1)))
    crossed = parts_dot(image1, joined(two_parts(direction), image1), 0, 0)
    curv1 = summed_halves(crossed[:, :LANES])
    upper, lower = squares_of(
        0.5 * (curv1 + curv1.T),
        summed_halves(gram_of(two_parts(residual))),
        summed_halves(crossed[:, LANES:]),
    )
    lines[0:32] = folded(upper)
    lines[32:64] = folded(lower)
    start = pl.multiple_of(lax.axis_index(COL[-1]) * 16, 16)
    part = jnp.concatenate([lines[pl.ds(32 * m + start, 16)] for m in range(2)], axis=0)
    for place in range(share_ref.shape[0]):
        for quad in range(8):
            share_ref[place, quad] = part[4 * quad : 4 * quad + 4]
    coef_ref[0:64] = jnp.concatenate([coef0, dcoef], axis=1)
    coef_ref[64:128] = jnp.concatenate([gram, eye], axis=1)


def middle(units, rhs, image, noise, rows):
    return pl.pallas_call(
        middle_kernel,
        in_specs=[VMEM] * 4,
        out_specs=[VMEM] * 3,
        out_shape=[
            jax.ShapeDtypeStruct((rows, 8, 4, LANES), F32),
            jax.ShapeDtypeStruct(rhs.shape, F32),
            jax.ShapeDtypeStruct((128, LANES), F32),
        ],
        scratch_shapes=[pltpu.VMEM((96, LANES), F32)],
        compiler_params=PARAMS,
        name="middle",
    )(units, rhs, image, noise)


def final_kernel(lines_ref, coef_ref, rhs_ref, packed_ref, image_ref, second_ref, sol_ref, res_ref, norm_ref):
    low = lane_of((32, LANES)) < HALF
    upper, lower = (
        unfolded(
            jnp.concatenate(
                [lines_ref[half, 4 * m + quad] for half in range(2) for quad in range(4)], axis=0
            )
        )
        for m in range(2)
    )
    curv1, gram1, square = matrices_of(upper, lower)
    coef0, dcoef = coef_ref[0:64, :HALF], coef_ref[0:64, HALF:]
    gram, eye = coef_ref[64:128, :HALF], coef_ref[64:128, HALF:]
    (coef1,) = solve_sym((curv1, gram1))
    cross = small_dot(curv1, coef1)
    gram2 = gram1 - cross - cross.T + small_dot(coef1.T, small_dot(square, coef1))
    norms = jnp.sum(eye * gram2, axis=0, keepdims=True) / jnp.sum(eye * gram, axis=0, keepdims=True)
    norm_ref[...] = jnp.sqrt(jnp.maximum(norms, 0.0))
    linear = coef0 + coef1 + small_dot(dcoef, coef1)
    quadratic = small_dot(coef0, coef1)
    scaled = quadratic * (1.0 / THETA)

    def doubled(first, second):
        first, second = first.T, second.T
        high, rest = two_parts(jnp.concatenate([first, first, second, second], axis=1))
        return jnp.concatenate([high, rest], axis=0)

    sol_c = doubled(linear, -quadratic)
    res_c = doubled(linear - scaled, scaled)

    def spread(ref, start):
        pieces = []
        for part in range(4):
            rows = ref[start // 2 + part * 32 : start // 2 + part * 32 + 32]
            pieces += [jnp.where(low, rows, 0.0), jnp.where(low, 0.0, rows)]
        return two_parts(jnp.concatenate(pieces, axis=0))

    def mixed(coefs, pair):
        both = bf16_dot(coefs, pair[0], 1, 1)
        return both[:HALF] + both[HALF:] + bf16_dot(coefs[:HALF], pair[1], 1, 1)

    for start in range(0, rhs_ref.shape[1], 256):
        cut = slice(start, start + 256)
        image = spread(image_ref, start)
        sol_ref[:, cut] = mixed(sol_c, joined(spread(packed_ref, start), image))
        res_ref[:, cut] = rhs_ref[:, cut] - mixed(res_c, joined(image, spread(second_ref, start)))


def final_outputs(lines, coefs, right_sides, rhs, image, second):
    return pl.pallas_call(
        final_kernel,
        in_specs=[VMEM] * 6,
        out_specs=[VMEM] * 3,
        out_shape=[jax.ShapeDtypeStruct(right_sides.shape, F32)] * 2
        + [jax.ShapeDtypeStruct((1, HALF), F32)],
        compiler_params=PARAMS,
        name="final_outputs",
    )(lines, coefs, right_sides, rhs, image, second)


def exchanged(parts, axis):
    return lax.all_to_all(parts, axis, 0, 0, tiled=True)


def shared(value, axis):
    return exchanged(jnp.broadcast_to(value[None], (lax.axis_size(axis), *value.shape)), axis)


def on_device(points, noise_level, right_sides):
    rows, cols = lax.axis_size("row"), lax.axis_size(COL)
    row_units, col_units = own_units(points, rows, cols)
    col_pts = exchanged(col_units, COL)
    row_pts = exchanged(row_units, "row")
    rhs, noise = prepare(right_sides, noise_level)

    part = first_product(row_pts, col_pts, rhs)
    own = jnp.sum(exchanged(part, "row"), axis=0)
    raw = shared(own, COL)
    part, image = second_product(row_pts, col_pts, raw, rhs, noise)
    own = jnp.sum(exchanged(part, "row"), axis=0)
    share, second, coefs = middle(shared(own, COL), rhs, image, noise, rows)
    lines = lax.all_gather(jnp.sum(exchanged(share, "row"), axis=0), COL[-1])
    sol, res, norms = final_outputs(lines, coefs, right_sides, rhs, image, second)
    return sol, res, norms[0]


def solution(mesh):
    torus = Mesh(
        mesh.devices.reshape(mesh.shape["row"], 4, 4, 2), ("row", "col_0", "col_1", "col_2")
    )
    return jax.shard_map(
        on_device,
        mesh=torus,
        in_specs=(P(None, ROW_COL), P("row"), P(None, "row")),
        out_specs=(P(None, "row"), P(None, "row"), P()),
        check_vma=False,
    )
```
